8 devices in a mesh: dp: 1 (over z), yz: 2 (over y), x: 4 (over x, core).
Axes of the slice: x: 2, y: 2, z: 1, core: 2. Of those that a mesh axis runs over, the one named last changes fastest.
Arguments:
- hidden: bfloat16 [64, 4096], P('dp', ('x', 'yz'))
- norm_gain: bfloat16 [3, 4096], P(None, 'x')
- w_q: bfloat16 [3, 4096, 4096], P(None, 'x', 'yz')
- w_kv: bfloat16 [3, 4096, 512], P(None, 'x', 'yz')
- w_gate: bfloat16 [3, 4096, 16384], P(None, 'x', 'yz')
- w_up: bfloat16 [3, 4096, 16384], P(None, 'x', 'yz')
- w_o: bfloat16 [3, 4096, 4096], P(None, 'yz', 'x')
- w_down: bfloat16 [3, 16384, 4096], P(None, 'yz', 'x')
- k_cache: bfloat16 [3, 64, 256, 256], P(None, ('dp', 'x', 'yz'))
- v_cache: bfloat16 [3, 64, 256, 256], P(None, ('dp', 'x', 'yz'))
- seq_len: int32 [64], P(('dp', 'x', 'yz'))
Outputs:
- output 1: bfloat16 [64, 4096], P('dp', ('x', 'yz'))
- output 2: bfloat16 [3, 64, 256, 256], P(None, ('dp', 'x', 'yz'))
- output 3: bfloat16 [3, 64, 256, 256], P(None, ('dp', 'x', 'yz'))
All inputs are finite; a program needn't handle non-finite values.
Results may differ from the reference program's by a relative error of at most 0.02.
Values are sent between devices in bfloat16 or wider.
A program may use at most 1 GiB of HBM per device.

```python
import math
import jax
import jax.numpy as jnp
from jax import lax

D_MODEL = 4096
N_HEADS = 16
HEAD_DIM = 256
D_FF = 16384
LAYERS = 3
BATCH_SIZE = 64
CACHE_LEN = 256

NORM_EPS = 1e-6
QUERY_COLS = N_HEADS * HEAD_DIM
KEY_SCALE = math.sqrt(math.log(CACHE_LEN / 16.0))


def setup_inputs(seed: int = 0, part: int = 0) -> dict:
    base_key = jax.random.key(seed)
    shared = jax.random.split(base_key, 7)
    part_keys = jax.random.split(jax.random.fold_in(base_key, part), 5)
    col_ramp = 0.4 + 1.2 * jnp.arange(D_MODEL, dtype=jnp.float32) / D_MODEL
    hidden = jax.random.normal(part_keys[0], (BATCH_SIZE, D_MODEL), jnp.float32) * col_ramp
    norm_gain = 1.0 + 0.4 * jax.random.normal(shared[0], (LAYERS, D_MODEL), jnp.float32)
    w_q = jax.random.normal(shared[1], (LAYERS, D_MODEL, QUERY_COLS), jnp.float32) * D_MODEL ** -0.5
    kv_scale = jnp.concatenate([jnp.full((HEAD_DIM,), KEY_SCALE, jnp.float32), jnp.ones((HEAD_DIM,), jnp.float32)])
    w_kv = jax.random.normal(shared[2], (LAYERS, D_MODEL, 2 * HEAD_DIM), jnp.float32) * kv_scale * D_MODEL ** -0.5
    w_gate = jax.random.normal(shared[3], (LAYERS, D_MODEL, D_FF), jnp.float32) * D_MODEL ** -0.5
    w_up = jax.random.normal(shared[4], (LAYERS, D_MODEL, D_FF), jnp.float32) * D_MODEL ** -0.5
    w_o = jax.random.normal(shared[5], (LAYERS, QUERY_COLS, D_MODEL), jnp.float32) * 2.0 * QUERY_COLS ** -0.5
    w_down = jax.random.normal(shared[6], (LAYERS, D_FF, D_MODEL), jnp.float32) * 1.5 * D_FF ** -0.5
    k_cache = jax.random.normal(part_keys[1], (LAYERS, BATCH_SIZE, CACHE_LEN, HEAD_DIM), jnp.float32) * KEY_SCALE
    v_cache = jax.random.normal(part_keys[2], (LAYERS, BATCH_SIZE, CACHE_LEN, HEAD_DIM), jnp.float32)
    drawn_len = jax.random.randint(part_keys[3], (BATCH_SIZE,), 1, CACHE_LEN, dtype=jnp.int32)
    longest_at = jax.random.randint(part_keys[4], (), 0, BATCH_SIZE, dtype=jnp.int32)
    seq_len = jnp.where(jnp.arange(BATCH_SIZE) == longest_at, CACHE_LEN - 1, drawn_len).astype(jnp.int32)
    return {
        "hidden": hidden.astype(jnp.bfloat16),
        "norm_gain": norm_gain.astype(jnp.bfloat16),
        "w_q": w_q.astype(jnp.bfloat16),
        "w_kv": w_kv.astype(jnp.bfloat16),
        "w_gate": w_gate.astype(jnp.bfloat16),
        "w_up": w_up.astype(jnp.bfloat16),
        "w_o": w_o.astype(jnp.bfloat16),
        "w_down": w_down.astype(jnp.bfloat16),
        "k_cache": k_cache.astype(jnp.bfloat16),
        "v_cache": v_cache.astype(jnp.bfloat16),
        "seq_len": seq_len,
    }


def rms_scale(hidden, norm_gain):
    hidden_f32 = hidden.astype(jnp.float32)
    inv_rms = lax.rsqrt(jnp.mean(hidden_f32 * hidden_f32, axis=-1, keepdims=True) + NORM_EPS)
    return (hidden_f32 * inv_rms * norm_gain.astype(jnp.float32)).astype(jnp.bfloat16)


def attend_one(packed):
    query_row, keys_row, values_row, length = packed
    scores = jnp.dot(query_row, keys_row.T, preferred_element_type=jnp.float32) * HEAD_DIM ** -0.5
    visible = jnp.arange(CACHE_LEN) <= length
    scores = jnp.where(visible[None, :], scores, -1e30)
    weights = jnp.exp(scores - jnp.max(scores, axis=-1, keepdims=True))
    probs_bf = (weights / jnp.sum(weights, axis=-1, keepdims=True)).astype(jnp.bfloat16)
    return jnp.dot(probs_bf, values_row, preferred_element_type=jnp.float32).astype(jnp.bfloat16)


def reference(hidden, norm_gain, w_q, w_kv, w_gate, w_up, w_o, w_down, k_cache, v_cache, seq_len):
    slot_hit = (jnp.arange(CACHE_LEN)[None, :] == seq_len[:, None])[:, :, None]

    def layer_step(residual, layer_args):
        l_gain, l_wq, l_wkv, l_wgate, l_wup, l_wo, l_wdown, l_kc, l_vc = layer_args
        normed = rms_scale(residual, l_gain)
        query_heads = jnp.dot(normed, l_wq, preferred_element_type=jnp.float32).astype(jnp.bfloat16).reshape(BATCH_SIZE, N_HEADS, HEAD_DIM)
        kv_new = jnp.dot(normed, l_wkv, preferred_element_type=jnp.float32).astype(jnp.bfloat16)
        gate_act = jnp.dot(normed, l_wgate, preferred_element_type=jnp.float32).astype(jnp.bfloat16)
        up_act = jnp.dot(normed, l_wup, preferred_element_type=jnp.float32).astype(jnp.bfloat16)
        new_k = jnp.where(slot_hit, kv_new[:, None, :HEAD_DIM], l_kc)
        new_v = jnp.where(slot_hit, kv_new[:, None, HEAD_DIM:], l_vc)
        attn_out = lax.map(attend_one, (query_heads, new_k, new_v, seq_len))
        mlp_act = (jax.nn.silu(gate_act.astype(jnp.float32)) * up_act.astype(jnp.float32)).astype(jnp.bfloat16)
        update = jnp.dot(attn_out.reshape(BATCH_SIZE, QUERY_COLS), l_wo, preferred_element_type=jnp.float32) + jnp.dot(mlp_act, l_wdown, preferred_element_type=jnp.float32)
        return (residual.astype(jnp.float32) + update).astype(jnp.bfloat16), (new_k, new_v)

    hidden_out, (k_out, v_out) = lax.scan(layer_step, hidden, (norm_gain, w_q, w_kv, w_gate, w_up, w_o, w_down, k_cache, v_cache))
    return hidden_out, k_out, v_out
```

```python
import functools

import jax
import jax.numpy as jnp
from jax import lax
from jax.experimental import pallas as pl
from jax.experimental.pallas import tpu as pltpu
from jax.sharding import PartitionSpec as P

NORM_EPS = 1e-6
MESH = pl.DeviceIdType.MESH
BF = jnp.bfloat16
F32 = jnp.float32

NG = 7
ND = 7
LAG_B, LAG_C, LAG_D, LAG_E = 1, 3, 5, 6


def step_kernel(dims, hid, gain, wq, wkv, wg, wu, wo, wd, kc, vc, lens,
                hout, knew, vnew,
                wq_b, wkv_b, wg_b, wu_b, wo_b, wd_b, k_b, v_b,
                hin, h_b, u_b, acc, ss_s, ss_r,
                part, rb, ib, m_all, part_q, rb_q, ib_q, zq, yq, ob, o_all, yx_s, yx_r,
                sem_wq, sem_wkv, sem_g, sem_u, sem_wo, sem_d, sem_k, sem_v,
                sem_h, sem_ss, sem_rb, sem_ib, sem_mp, sem_mq, sem_mf,
                sem_zq, sem_oy, sem_op, sem_oq, sem_of, sem_yx):
    L, CH, NCH, D = dims["layers"], dims["chunk"], dims["n_chunks"], dims["d"]
    HD = 256
    QC = wq_b.shape[1]
    x = lax.axis_index("x")
    y = lax.axis_index("yz")
    c = lax.rem(x, 2)
    cx = x // 2
    xp = x + 1 - 2 * c
    xq = lax.rem(x + 2, 4)
    xd = 3 - x
    dev_p, dev_q, dev_d, dev_y = {"x": xp}, {"x": xq}, {"x": xd}, {"yz": 1 - y}

    def rc(src, dst, sems, dev):
        return pltpu.make_async_remote_copy(
            src_ref=src, dst_ref=dst, send_sem=sems[0], recv_sem=sems[1],
            device_id=dev, device_id_type=MESH)

    def sp(s, *idx):
        return (s.at[(0,) + idx], s.at[(1,) + idx])

    def cp_q(l):
        return (pltpu.make_async_copy(wq.at[l], wq_b, sem_wq),
                pltpu.make_async_copy(wkv.at[l], wkv_b, sem_wkv))

    def cp_gu(i):
        l, j, s = i // NCH, lax.rem(i, NCH), lax.rem(i, NG)
        cols = pl.ds(pl.multiple_of(j * CH, CH), CH)
        return (pltpu.make_async_copy(wg.at[l, :, cols], wg_b.at[s], sem_g.at[s]),
                pltpu.make_async_copy(wu.at[l, :, cols], wu_b.at[s], sem_u.at[s]))

    def cp_d(i):
        l, j, s = i // NCH, lax.rem(i, NCH), lax.rem(i, ND)
        rows = pl.ds(pl.multiple_of(j * CH, CH), CH)
        return (pltpu.make_async_copy(wd.at[l, rows, :], wd_b.at[s], sem_d.at[s]),)

    def cp_o(l):
        return (pltpu.make_async_copy(wo.at[l], wo_b, sem_wo),)

    def cp_kv(l):
        return (pltpu.make_async_copy(kc.at[l], k_b, sem_k),
                pltpu.make_async_copy(vc.at[l], v_b, sem_v))

    def start(cs):
        for cpy in cs:
            cpy.start()

    def wait(cs):
        for cpy in cs:
            cpy.wait()

    start(cp_q(0))
    start(cp_gu(0))

    barrier = pltpu.get_barrier_semaphore()
    for dev in (dev_p, dev_q, dev_d, dev_y):
        pl.semaphore_signal(barrier, inc=1, device_id=dev, device_id_type=MESH)
    pl.semaphore_wait(barrier, 4)

    h_send = rc(hid, hin.at[y], sp(sem_h), dev_y)
    h_send.start()
    hin[y] = hid[...]
    start(cp_gu(1))
    rc(hid, hin.at[1 - y], sp(sem_h), dev_y).wait_recv()
    half = hid.shape[1]
    h_b[:, :half] = hin[0]
    h_b[:, half:] = hin[1]
    h_send.wait_send()

    rows = h_b.shape[0]
    eye = (lax.broadcasted_iota(jnp.int32, (rows, 128), 0)
           == lax.broadcasted_iota(jnp.int32, (rows, 128), 1))

    def norm(l):
        h = h_b[...].astype(F32)
        ss = jnp.sum(h * h, axis=1, keepdims=True)
        ss_row = jnp.sum(jnp.where(eye, ss, 0.0), axis=0, keepdims=True)
        ss_s[...] = jnp.broadcast_to(ss_row, ss_s.shape)
        cps = [rc(ss_s, ss_r.at[k], sp(sem_ss, k), dev)
               for k, dev in enumerate((dev_p, dev_q, dev_d))]
        for cpy in cps:
            cpy.start()
        gall = gain[...].astype(F32)
        g = gall[0:1]
        for k in range(1, L):
            g = jnp.where(l == k, gall[k:k + 1], g)
        for cpy in cps:
            cpy.wait()
        tot = (ss_s[0:1] + ss_r[0, 0:1]) + (ss_r[1, 0:1] + ss_r[2, 0:1])
        tot_col = jnp.sum(jnp.where(eye, jnp.broadcast_to(tot, eye.shape), 0.0), axis=1, keepdims=True)
        inv = lax.rsqrt(tot_col / D + NORM_EPS)
        u_b[...] = (h * inv * g).astype(BF)

    def put_rows(dst, cols, val):
        v = val.astype(BF)
        for r in range(4):
            dst[r // 2, r % 2, :, cols] = v[16 * r:16 * r + 16]

    def a_q(l):
        wait(cp_q(l))
        u = u_b[...]
        for n in range(0, QC, 512):
            put_rows(part_q, slice(n, n + 512), jnp.dot(u, wq_b[:, n:n + 512], preferred_element_type=F32))
        put_rows(part_q, slice(QC, QC + HD), jnp.dot(u, wkv_b[...], preferred_element_type=F32))
        rc(part_q.at[:, 1 - c], rb_q, sp(sem_rb, NCH), dev_p).start()

        @pl.when(l + 1 < L)
        def _():
            start(cp_q(l + 1))

    def b_q():
        rc(part_q.at[:, 1 - c], rb_q, sp(sem_rb, NCH), dev_p).wait()
        s = part_q[1 - cx, c].astype(F32) + rb_q[1 - cx].astype(F32)
        part_q[1 - cx, c] = s.astype(BF)
        rc(part_q.at[1 - cx, c], ib_q, sp(sem_ib, NCH), dev_q).start()

    def c_q():
        rc(part_q.at[1 - cx, c], ib_q, sp(sem_ib, NCH), dev_q).wait()
        z = (part_q[cx, c].astype(F32) + rb_q[cx].astype(F32)) + ib_q[...].astype(F32)
        zq[0] = z[0:8].astype(BF)
        zq[1] = z[8:16].astype(BF)
        rc(zq.at[1 - y], yq.at[y], sp(sem_zq), dev_y).start()
        yq[y] = zq[y]

    def attend(l):
        rc(zq.at[1 - y], yq.at[1 - y], sp(sem_zq), dev_y).wait()
        q0 = yq[0].astype(F32)
        q1 = yq[1].astype(F32)
        k_new = q0[:, QC:]
        v_new = q1[:, QC:]
        knew[l] = k_new.astype(BF)
        vnew[l] = v_new.astype(BF)
        nh = QC // HD
        ns = 8
        heads = [qq[:, h * HD:(h + 1) * HD] for qq in (q0, q1) for h in range(nh)]
        qf = jnp.concatenate(heads, axis=0)
        qb = qf.astype(BF)
        nr = 2 * nh * ns
        pos = lax.broadcasted_iota(jnp.int32, (nr, HD), 1)
        seq = lax.rem(lax.broadcasted_iota(jnp.int32, (nr, HD), 0), ns)
        ln = jnp.zeros((nr, HD), jnp.int32)
        for b in range(ns):
            ln = jnp.where(seq == b, lens[b], ln)
        k_rep = jnp.concatenate([k_new] * (2 * nh), axis=0)
        v_rep = jnp.concatenate([v_new] * (2 * nh), axis=0)
        s_new = jnp.sum(qf * k_rep, axis=1, keepdims=True)
        wait(cp_kv(l))
        s = jnp.zeros((nr, HD), F32)
        for b in range(ns):
            sb = lax.dot_general(qb, k_b[b], (((1,), (1,)), ((), ())), preferred_element_type=F32)
            s = jnp.where(seq == b, sb, s)
        s = jnp.where(pos == ln, s_new, s) * HD ** -0.5
        s = jnp.where(pos <= ln, s, -1e30)
        e = jnp.exp(s - jnp.max(s, axis=1, keepdims=True))
        p = (e / jnp.sum(e, axis=1, keepdims=True)).astype(BF).astype(F32)
        p_new = jnp.sum(jnp.where(pos == ln, p, 0.0), axis=1, keepdims=True)
        p_old = jnp.where(pos == ln, 0.0, p)
        o = p_new * v_rep
        for b in range(ns):
            pb = jnp.where(seq == b, p_old, 0.0).astype(BF)
            o = o + jnp.dot(pb, v_b[b], preferred_element_type=F32)
        for hh in range(2):
            for h in range(nh):
                r0 = (hh * nh + h) * ns
                ob[hh, :, h * HD:(h + 1) * HD] = o[r0:r0 + ns].astype(BF)
        rc(ob.at[1 - y], o_all.at[x, y], sp(sem_oy), dev_y).start()
        o_all[x, y] = ob[y]

        @pl.when(l + 1 < L)
        def _():
            start(cp_kv(l + 1))

    def o_send():
        rc(ob.at[1 - y], o_all.at[x, 1 - y], sp(sem_oy), dev_y).wait()
        rc(o_all.at[x], o_all.at[x], sp(sem_op), dev_p).start()
        rc(o_all.at[x], o_all.at[x], sp(sem_oq), dev_q).start()

    def o_fwd():
        rc(o_all.at[xq], o_all.at[xq], sp(sem_oq), dev_q).wait_recv()
        rc(o_all.at[xq], o_all.at[xq], sp(sem_of), dev_p).start()

    def e_o(l):
        rc(o_all.at[x], o_all.at[xp], sp(sem_op), dev_p).wait()
        rc(o_all.at[xq], o_all.at[xd], sp(sem_of), dev_p).wait()
        rc(o_all.at[x], o_all.at[x], sp(sem_oq), dev_q).wait_send()
        wait(cp_o(l))
        blocks = [o_all[i // 2, i % 2].astype(F32) for i in range(8)]
        lhs = jnp.concatenate(blocks, axis=0).astype(BF)
        for n in range(0, acc.shape[1], 512):
            acc[:, n:n + 512] += jnp.dot(lhs, wo_b[:, n:n + 512], preferred_element_type=F32)

        @pl.when(l + 1 < L)
        def _():
            start(cp_o(l + 1))

    def stage_a(l, j):
        i = l * NCH + j
        s = lax.rem(i, NG)
        wait(cp_gu(i))
        u = u_b[...]
        dst = part.at[j]
        for n in range(0, CH, 512):
            put_rows(dst, slice(n, n + 512), jnp.dot(u, wg_b[s, :, n:n + 512], preferred_element_type=F32))
            put_rows(dst, slice(CH + n, CH + n + 512), jnp.dot(u, wu_b[s, :, n:n + 512], preferred_element_type=F32))
        rc(part.at[j, :, 1 - c], rb.at[j], sp(sem_rb, j), dev_p).start()

        @pl.when(i + NG < L * NCH)
        def _():
            start(cp_gu(i + NG))

    def stage_b(j):
        rc(part.at[j, :, 1 - c], rb.at[j], sp(sem_rb, j), dev_p).wait()
        s = part[j, 1 - cx, c].astype(F32) + rb[j, 1 - cx].astype(F32)
        part[j, 1 - cx, c] = s.astype(BF)
        rc(part.at[j, 1 - cx, c], ib.at[j], sp(sem_ib, j), dev_q).start()

    def stage_c(j):
        rc(part.at[j, 1 - cx, c], ib.at[j], sp(sem_ib, j), dev_q).wait()
        z = (part[j, cx, c].astype(F32) + rb[j, cx].astype(F32)) + ib[j].astype(F32)
        z = z.astype(BF).astype(F32)
        gate, up = z[:, :CH], z[:, CH:]
        m_all[j, x] = (jax.nn.silu(gate) * up).astype(BF)
        rc(m_all.at[j, x], m_all.at[j, x], sp(sem_mq, j), dev_q).start()
        rc(m_all.at[j, x], m_all.at[j, x], sp(sem_mp, j), dev_p).start()

    def stage_d(j):
        rc(m_all.at[j, xq], m_all.at[j, xq], sp(sem_mq, j), dev_q).wait_recv()
        rc(m_all.at[j, xq], m_all.at[j, xq], sp(sem_mf, j), dev_p).start()

    def stage_e(l, j):
        i = l * NCH + j
        s = lax.rem(i, ND)
        rc(m_all.at[j, x], m_all.at[j, xp], sp(sem_mp, j), dev_p).wait()
        rc(m_all.at[j, xq], m_all.at[j, xd], sp(sem_mf, j), dev_p).wait()
        rc(m_all.at[j, x], m_all.at[j, x], sp(sem_mq, j), dev_q).wait_send()
        wait(cp_d(i))
        m = m_all[j].reshape(rows, CH)
        for n in range(0, acc.shape[1], 512):
            acc[:, n:n + 512] += jnp.dot(m, wd_b[s, :, n:n + 512], preferred_element_type=F32)

        @pl.when(i + ND < L * NCH)
        def _():
            start(cp_d(i + ND))

    def layer(l, carry):
        norm(l)
        acc[...] = jnp.zeros_like(acc)
        a_q(l)

        def step(t, carry2):
            @pl.when((l == 0) & (t + 2 < NG))
            def _():
                start(cp_gu(t + 2))

            @pl.when(t < NCH)
            def _():
                stage_a(l, t)

            @pl.when((l == 0) & (t < ND))
            def _():
                start(cp_d(t))

            @pl.when(t == 0)
            def _():
                @pl.when(l == 0)
                def _():
                    start(cp_kv(0))
                b_q()

            @pl.when(t == 1)
            def _():
                @pl.when(l == 0)
                def _():
                    start(cp_o(0))

            @pl.when((t >= LAG_B) & (t < NCH + LAG_B))
            def _():
                stage_b(t - LAG_B)

            @pl.when(t == 2)
            def _():
                c_q()

            @pl.when((t >= LAG_C) & (t < NCH + LAG_C))
            def _():
                stage_c(t - LAG_C)

            @pl.when(t == 4)
            def _():
                attend(l)

            @pl.when(t == 6)
            def _():
                o_send()

            @pl.when((t >= LAG_D) & (t < NCH + LAG_D))
            def _():
                stage_d(t - LAG_D)

            @pl.when(t == 8)
            def _():
                o_fwd()

            @pl.when((t >= LAG_E) & (t < NCH + LAG_E))
            def _():
                stage_e(l, t - LAG_E)

            @pl.when(t == 10)
            def _():
                e_o(l)
            return carry2

        lax.fori_loop(0, NCH + LAG_E, step, 0)

        yx_s[...] = acc[...].astype(BF)
        yx = rc(yx_s, yx_r, sp(sem_yx), dev_y)
        yx.start()
        yx.wait()
        h_b[...] = (h_b[...].astype(F32) + (yx_s[...].astype(F32) + yx_r[...].astype(F32))).astype(BF)
        return carry

    lax.fori_loop(0, L, layer, 0)
    hout[...] = h_b[:, pl.ds(pl.multiple_of(y * half, half), half)]


def solution(mesh):
    row_spec = P("dp", ("x", "yz"))
    tile_in = P(None, "x", "yz")
    tile_out = P(None, "yz", "x")
    cache_spec = P(None, ("dp", "x", "yz"))
    len_spec = P(("dp", "x", "yz"))

    def device_step(hidden, norm_gain, w_q, w_kv, w_gate, w_up, w_o, w_down, k_cache, v_cache, seq_len):
        L, k_in, q_cols = w_q.shape
        rows = hidden.shape[0]
        half = hidden.shape[1]
        kv_cols = w_kv.shape[2]
        ff = w_gate.shape[2]
        ch = 1024
        nch = ff // ch
        d_out = w_o.shape[2]
        ns, cache_len, hd = k_cache.shape[1:]
        zc = q_cols + kv_cols
        dims = {"layers": L, "chunk": ch, "n_chunks": nch, "d": half * 8}
        vm = pl.BlockSpec(memory_space=pltpu.VMEM)
        anyspec = pl.BlockSpec(memory_space=pl.ANY)
        DMA = pltpu.SemaphoreType.DMA
        V = pltpu.VMEM
        h_new, k_new, v_new = pl.pallas_call(
            functools.partial(step_kernel, dims),
            out_shape=(
                jax.ShapeDtypeStruct(hidden.shape, BF),
                jax.ShapeDtypeStruct((L, ns, hd), BF),
                jax.ShapeDtypeStruct((L, ns, hd), BF),
            ),
            in_specs=[vm, vm] + [anyspec] * 8 + [pl.BlockSpec(memory_space=pltpu.SMEM)],
            out_specs=(vm, vm, vm),
            scratch_shapes=[
                V((k_in, q_cols), BF), V((k_in, kv_cols), BF),
                V((NG, k_in, ch), BF), V((NG, k_in, ch), BF),
                V((q_cols, d_out), BF), V((ND, ch, d_out), BF),
                V((ns, cache_len, hd), BF), V((ns, cache_len, hd), BF),
                V((2, rows, half), BF), V((rows, d_out), BF), V((rows, d_out), BF), V((rows, d_out), F32),
                V((8, 128), F32), V((3, 8, 128), F32),
                V((nch, 2, 2, 16, 2 * ch), BF), V((nch, 2, 16, 2 * ch), BF), V((nch, 16, 2 * ch), BF),
                V((nch, 4, 16, ch), BF),
                V((2, 2, 16, zc), BF), V((2, 16, zc), BF), V((16, zc), BF),
                V((2, ns, zc), BF), V((2, ns, zc), BF),
                V((2, ns, q_cols), BF), V((4, 2, ns, q_cols), BF),
                V((rows, d_out), BF), V((rows, d_out), BF),
                DMA, DMA, DMA((NG,)), DMA((NG,)), DMA, DMA((ND,)), DMA, DMA,
                DMA((2,)), DMA((2, 3)), DMA((2, nch + 1)), DMA((2, nch + 1)),
                DMA((2, nch)), DMA((2, nch)), DMA((2, nch)),
                DMA((2,)), DMA((2,)), DMA((2,)), DMA((2,)), DMA((2,)), DMA((2,)),
            ],
            compiler_params=pltpu.CompilerParams(
                collective_id=0, has_side_effects=True, vmem_limit_bytes=67_000_000),
            name="decode_step",
        )(hidden, norm_gain, w_q, w_kv, w_gate, w_up, w_o, w_down, k_cache, v_cache, seq_len)
        slot_hit = (jnp.arange(cache_len)[None, :] == seq_len[:, None])[None, :, :, None]
        k_out = jnp.where(slot_hit, k_new[:, :, None, :], k_cache)
        v_out = jnp.where(slot_hit, v_new[:, :, None, :], v_cache)
        return h_new, k_out, v_out

    return jax.shard_map(
        device_step,
        mesh=mesh,
        in_specs=(row_spec, P(None, "x"), tile_in, tile_in, tile_in, tile_in, tile_out, tile_out, cache_spec, cache_spec, len_spec),
        out_specs=(row_spec, cache_spec, cache_spec),
        check_vma=False,
    )
```

```python
import functools

import jax
import jax.numpy as jnp
from jax import lax
from jax.experimental import pallas as pl
from jax.experimental.pallas import tpu as pltpu
from jax.sharding import PartitionSpec as P

NORM_EPS = 1e-6
MESH = pl.DeviceIdType.MESH
BF = jnp.bfloat16
F32 = jnp.float32

CH = 1024
NG = 7
ND = 8
T_B = (1, 2, 3, 4, 5, 6, 7, 8)
T_C = (5, 7, 8, 9, 10, 11, 12, 13)
T_D = (11, 13, 14, 15, 16, 18, 19)
T_EN = (8, 9, 10, 11, 12, 13, 14)
T_EF = (12, 14, 15, 16, 17, 19, 20)
T_QB, T_QC, T_ATT, T_OS, T_ON, T_OF, T_OE, T_LN = 0, 4, 7, 11, 12, 17, 18, 14
STEPS = 21


def step_kernel(dims, hid, gain, wq, wkv, wg, wu, wo, wd, kc, vc, lens,
                hout, knew, vnew,
                wq_b, wkv_b, wg_b, wu_b, wo_b, wd_b, k_b, v_b,
                hin, h_b, u_b, acc, ss_s, ss_r,
                part, rb, ib, m_all, part_q, rb_q, ib_q, zq, yq, ob, o_all, yx_s, yx_r,
                sem_wq, sem_wkv, sem_g, sem_u, sem_wo, sem_d, sem_k, sem_v,
                sem_h, sem_ss, sem_rb, sem_ib, sem_mp, sem_mq, sem_mf,
                sem_zq, sem_oy, sem_op, sem_oq, sem_of, sem_yx):
    L, NCH, D = dims["layers"], dims["n_chunks"], dims["d"]
    HD = 256
    QC = wq_b.shape[1]
    x = lax.axis_index("x")
    y = lax.axis_index("yz")
    c = lax.rem(x, 2)
    cx = x // 2
    xp = x + 1 - 2 * c
    xq = lax.rem(x + 2, 4)
    xd = 3 - x
    dev_p, dev_q, dev_d, dev_y = {"x": xp}, {"x": xq}, {"x": xd}, {"yz": 1 - y}

    def rc(src, dst, sems, dev):
        return pltpu.make_async_remote_copy(
            src_ref=src, dst_ref=dst, send_sem=sems[0], recv_sem=sems[1],
            device_id=dev, device_id_type=MESH)

    def sp(s, *idx):
        return (s.at[(0,) + idx], s.at[(1,) + idx])

    def cp_q(l):
        return (pltpu.make_async_copy(wq.at[l], wq_b, sem_wq),
                pltpu.make_async_copy(wkv.at[l], wkv_b, sem_wkv))

    def cp_gu(i):
        l, j, s = i // NCH, lax.rem(i, NCH), lax.rem(i, NG)
        cols = pl.ds(pl.multiple_of(j * CH, CH), CH)
        return (pltpu.make_async_copy(wg.at[l, :, cols], wg_b.at[s], sem_g.at[s]),
                pltpu.make_async_copy(wu.at[l, :, cols], wu_b.at[s], sem_u.at[s]))

    def cp_d(i):
        l, j, s = i // NCH, lax.rem(i, NCH), lax.rem(i, ND)
        rows = pl.ds(pl.multiple_of(j * CH, CH), CH)
        return (pltpu.make_async_copy(wd.at[l, rows, :], wd_b.at[s], sem_d.at[s]),)

    def cp_o(l):
        return (pltpu.make_async_copy(wo.at[l], wo_b, sem_wo),)

    def cp_kv(l):
        return (pltpu.make_async_copy(kc.at[l], k_b, sem_k),
                pltpu.make_async_copy(vc.at[l], v_b, sem_v))

    def start(cs):
        for cpy in cs:
            cpy.start()

    def wait(cs):
        for cpy in cs:
            cpy.wait()

    start(cp_q(0))
    for k in range(4):
        start(cp_gu(k))

    with jax.named_scope("barrier"):
        barrier = pltpu.get_barrier_semaphore()
        for dev in (dev_p, dev_q, dev_d, dev_y):
            pl.semaphore_signal(barrier, inc=1, device_id=dev, device_id_type=MESH)
        pl.semaphore_wait(barrier, 4)

    with jax.named_scope("hx"):
        h_send = rc(hid, hin.at[y], sp(sem_h), dev_y)
        h_send.start()
        for k in range(4, NG):
            start(cp_gu(k))
        start(cp_kv(0))
        hin[y] = hid[...]
        rc(hid, hin.at[1 - y], sp(sem_h), dev_y).wait_recv()
        half = hid.shape[1]
        h_b[:, :half] = hin[0]
        h_b[:, half:] = hin[1]
        h_send.wait_send()

    rows = h_b.shape[0]
    eye = (lax.broadcasted_iota(jnp.int32, (rows, 128), 0)
           == lax.broadcasted_iota(jnp.int32, (rows, 128), 1))

    @jax.named_scope("norm")
    def norm(l):
        h = h_b[...].astype(F32)
        ss = jnp.sum(h * h, axis=1, keepdims=True)
        ss_row = jnp.sum(jnp.where(eye, ss, 0.0), axis=0, keepdims=True)
        ss_s[...] = jnp.broadcast_to(ss_row, ss_s.shape)
        cps = [rc(ss_s, ss_r.at[k], sp(sem_ss, k), dev)
               for k, dev in enumerate((dev_p, dev_q, dev_d))]
        for cpy in cps:
            cpy.start()
        gall = gain[...].astype(F32)
        g = gall[0:1]
        for k in range(1, L):
            g = jnp.where(l == k, gall[k:k + 1], g)
        for cpy in cps:
            cpy.wait()
        tot = (ss_s[0:1] + ss_r[0, 0:1]) + (ss_r[1, 0:1] + ss_r[2, 0:1])
        tot_col = jnp.sum(jnp.where(eye, jnp.broadcast_to(tot, eye.shape), 0.0), axis=1, keepdims=True)
        inv = lax.rsqrt(tot_col / D + NORM_EPS)
        u_b[...] = (h * inv * g).astype(BF)

    def put_rows(dst, cols, val):
        v = val.astype(BF)
        for r in range(4):
            dst[r // 2, r % 2, :, cols] = v[16 * r:16 * r + 16]

    @jax.named_scope("a_q")
    def a_q(l):
        wait(cp_q(l))
        u = u_b[...]
        for n in range(0, QC, 512):
            put_rows(part_q, slice(n, n + 512), jnp.dot(u, wq_b[:, n:n + 512], preferred_element_type=F32))
        put_rows(part_q, slice(QC, QC + HD), jnp.dot(u, wkv_b[...], preferred_element_type=F32))
        rc(part_q.at[:, 1 - c], rb_q, sp(sem_rb, NCH), dev_p).start()

        @pl.when(l + 1 < L)
        def _():
            start(cp_q(l + 1))

    @jax.named_scope("b_q")
    def b_q():
        rc(part_q.at[:, 1 - c], rb_q, sp(sem_rb, NCH), dev_p).wait()
        s = part_q[1 - cx, c].astype(F32) + rb_q[1 - cx].astype(F32)
        part_q[1 - cx, c] = s.astype(BF)
        rc(part_q.at[1 - cx, c], ib_q, sp(sem_ib, NCH), dev_q).start()

    @jax.named_scope("c_q")
    def c_q():
        rc(part_q.at[1 - cx, c], ib_q, sp(sem_ib, NCH), dev_q).wait()
        z = (part_q[cx, c].astype(F32) + rb_q[cx].astype(F32)) + ib_q[...].astype(F32)
        zq[0] = z[0:8].astype(BF)
        zq[1] = z[8:16].astype(BF)
        rc(zq.at[1 - y], yq.at[y], sp(sem_zq), dev_y).start()
        yq[y] = zq[y]

    @jax.named_scope("attend")
    def attend(l):
        rc(zq.at[1 - y], yq.at[1 - y], sp(sem_zq), dev_y).wait()
        q0 = yq[0].astype(F32)
        q1 = yq[1].astype(F32)
        k_new = q0[:, QC:]
        v_new = q1[:, QC:]
        knew[l] = k_new.astype(BF)
        vnew[l] = v_new.astype(BF)
        nh = QC // HD
        ns = 8
        heads = [qq[:, h * HD:(h + 1) * HD] for qq in (q0, q1) for h in range(nh)]
        qf = jnp.concatenate(heads, axis=0)
        qb = qf.astype(BF)
        nr = 2 * nh * ns
        pos = lax.broadcasted_iota(jnp.int32, (nr, HD), 1)
        seq = lax.rem(lax.broadcasted_iota(jnp.int32, (nr, HD), 0), ns)
        ln = jnp.zeros((nr, HD), jnp.int32)
        for b in range(ns):
            ln = jnp.where(seq == b, lens[b], ln)
        k_rep = jnp.concatenate([k_new] * (2 * nh), axis=0)
        v_rep = jnp.concatenate([v_new] * (2 * nh), axis=0)
        s_new = jnp.sum(qf * k_rep, axis=1, keepdims=True)
        wait(cp_kv(l))
        s = jnp.zeros((nr, HD), F32)
        for b in range(ns):
            sb = lax.dot_general(qb, k_b[b], (((1,), (1,)), ((), ())), preferred_element_type=F32)
            s = jnp.where(seq == b, sb, s)
        s = jnp.where(pos == ln, s_new, s) * HD ** -0.5
        s = jnp.where(pos <= ln, s, -1e30)
        e = jnp.exp(s - jnp.max(s, axis=1, keepdims=True))
        p = (e / jnp.sum(e, axis=1, keepdims=True)).astype(BF).astype(F32)
        p_new = jnp.sum(jnp.where(pos == ln, p, 0.0), axis=1, keepdims=True)
        p_old = jnp.where(pos == ln, 0.0, p)
        o = p_new * v_rep
        for b in range(ns):
            pb = jnp.where(seq == b, p_old, 0.0).astype(BF)
            o = o + jnp.dot(pb, v_b[b], preferred_element_type=F32)
        for hh in range(2):
            for h in range(nh):
                r0 = (hh * nh + h) * ns
                ob[hh, :, h * HD:(h + 1) * HD] = o[r0:r0 + ns].astype(BF)
        rc(ob.at[1 - y], o_all.at[cx, c, y], sp(sem_oy), dev_y).start()
        o_all[cx, c, y] = ob[y]

        @pl.when(l + 1 < L)
        def _():
            start(cp_kv(l + 1))

    @jax.named_scope("o_send")
    def o_send():
        rc(ob.at[1 - y], o_all.at[cx, c, 1 - y], sp(sem_oy), dev_y).wait()
        rc(o_all.at[cx, c], o_all.at[cx, c], sp(sem_op), dev_p).start()
        rc(o_all.at[cx, c], o_all.at[cx, c], sp(sem_oq), dev_q).start()

    @jax.named_scope("o_fwd")
    def o_fwd():
        rc(o_all.at[1 - cx, c], o_all.at[1 - cx, c], sp(sem_oq), dev_q).wait_recv()
        rc(o_all.at[1 - cx, c], o_all.at[1 - cx, c], sp(sem_of), dev_p).start()

    def o_rows(g):
        blocks = [o_all[g, i // 2, i % 2].astype(F32) for i in range(4)]
        lhs = jnp.concatenate(blocks, axis=0).astype(BF)
        for n in range(0, acc.shape[2], 512):
            acc[g, :, n:n + 512] += jnp.dot(lhs, wo_b[:, n:n + 512], preferred_element_type=F32)

    @jax.named_scope("o_near")
    def o_near(l):
        rc(o_all.at[cx, c], o_all.at[cx, 1 - c], sp(sem_op), dev_p).wait()
        wait(cp_o(l))
        o_rows(cx)

    @jax.named_scope("o_far")
    def o_far(l):
        rc(o_all.at[1 - cx, c], o_all.at[1 - cx, 1 - c], sp(sem_of), dev_p).wait()
        rc(o_all.at[cx, c], o_all.at[cx, c], sp(sem_oq), dev_q).wait_send()
        o_rows(1 - cx)

        @pl.when(l + 1 < L)
        def _():
            start(cp_o(l + 1))

    @jax.named_scope("stage_a")
    def stage_a(l, j):
        i = l * NCH + j
        s = lax.rem(i, NG)
        wait(cp_gu(i))
        u = u_b[...]
        dst = part.at[j]
        for n in range(0, CH, 512):
            put_rows(dst, slice(n, n + 512), jnp.dot(u, wg_b[s, :, n:n + 512], preferred_element_type=F32))
            put_rows(dst, slice(CH + n, CH + n + 512), jnp.dot(u, wu_b[s, :, n:n + 512], preferred_element_type=F32))
        rc(part.at[j, :, 1 - c], rb.at[j], sp(sem_rb, j), dev_p).start()

        @pl.when(i + NG < L * NCH)
        def _():
            start(cp_gu(i + NG))

    @jax.named_scope("stage_b")
    def stage_b(j):
        rc(part.at[j, :, 1 - c], rb.at[j], sp(sem_rb, j), dev_p).wait()
        s = part[j, 1 - cx, c].astype(F32) + rb[j, 1 - cx].astype(F32)
        part[j, 1 - cx, c] = s.astype(BF)
        rc(part.at[j, 1 - cx, c], ib.at[j], sp(sem_ib, j), dev_q).start()

    @jax.named_scope("stage_c")
    def stage_c(j):
        rc(part.at[j, 1 - cx, c], ib.at[j], sp(sem_ib, j), dev_q).wait()
        z = (part[j, cx, c].astype(F32) + rb[j, cx].astype(F32)) + ib[j].astype(F32)
        z = z.astype(BF).astype(F32)
        gate, up = z[:, :CH], z[:, CH:]
        m_all[j, cx, c] = (jax.nn.silu(gate) * up).astype(BF)
        rc(m_all.at[j, cx, c], m_all.at[j, cx, c], sp(sem_mq, j), dev_q).start()
        rc(m_all.at[j, cx, c], m_all.at[j, cx, c], sp(sem_mp, j), dev_p).start()

    @jax.named_scope("stage_d")
    def stage_d(j):
        rc(m_all.at[j, 1 - cx, c], m_all.at[j, 1 - cx, c], sp(sem_mq, j), dev_q).wait_recv()
        rc(m_all.at[j, 1 - cx, c], m_all.at[j, 1 - cx, c], sp(sem_mf, j), dev_p).start()

    def e_rows(s, j, g):
        m = m_all[j, g].reshape(rows // 2, CH)
        for n in range(0, acc.shape[2], 512):
            acc[g, :, n:n + 512] += jnp.dot(m, wd_b[s, :, n:n + 512], preferred_element_type=F32)

    @jax.named_scope("e_near")
    def e_near(l, j):
        i = l * NCH + j
        rc(m_all.at[j, cx, c], m_all.at[j, cx, 1 - c], sp(sem_mp, j), dev_p).wait()
        wait(cp_d(i))
        e_rows(lax.rem(i, ND), j, cx)

    @jax.named_scope("e_far")
    def e_far(l, j):
        i = l * NCH + j
        rc(m_all.at[j, 1 - cx, c], m_all.at[j, 1 - cx, 1 - c], sp(sem_mf, j), dev_p).wait()
        rc(m_all.at[j, cx, c], m_all.at[j, cx, c], sp(sem_mq, j), dev_q).wait_send()
        e_rows(lax.rem(i, ND), j, 1 - cx)

        @pl.when(i + ND < L * NCH)
        def _():
            start(cp_d(i + ND))

    def layer(l, carry):
        norm(l)
        acc[...] = jnp.zeros_like(acc)
        a_q(l)

        def step(t, carry2):
            def at(steps, fn):
                if isinstance(steps, int):
                    pl.when(t == steps)(fn)
                    return
                hit = t == steps[0]
                j = jnp.int32(0)
                for k, st in enumerate(steps[1:]):
                    hit = hit | (t == st)
                    j = jnp.where(t >= st, k + 1, j)
                pl.when(hit)(lambda: fn(j))

            pl.when(t < NCH)(lambda: stage_a(l, t))
            pl.when((l == 0) & (t < ND))(lambda: start(cp_d(t)))
            pl.when((l == 0) & (t == 3))(lambda: start(cp_o(0)))
            at(T_QB, b_q)
            at(T_B, stage_b)
            at(T_QC, c_q)
            at(T_EN, lambda j: e_near(l, j))
            at(T_OS, o_send)
            at(T_D, stage_d)
            at(T_ON, lambda: o_near(l))
            at(T_OE, lambda: o_far(l))
            at(T_EF, lambda j: e_far(l, j))
            at(T_OF, o_fwd)
            at(T_C, stage_c)
            at(T_ATT, lambda: attend(l))
            at(T_LN, lambda: last_near(l))
            return carry2

        lax.fori_loop(0, STEPS, step, 0)

        stage_d(NCH - 1)
        last_far(l)
        swap(l)
        return carry

    def yx(g, n):
        return rc(yx_s.at[g, n], yx_r.at[g, n], sp(sem_yx, g, n), dev_y)

    def last_rows(s, g):
        m = m_all[NCH - 1, g].reshape(rows // 2, CH)
        for n in range(2):
            cols = slice(n * half, (n + 1) * half)
            v = acc[g, :, cols] + jnp.dot(m, wd_b[s, :, cols], preferred_element_type=F32)
            yx_s[g, n] = v.astype(BF)
            yx(g, n).start()

    @jax.named_scope("last_near")
    def last_near(l):
        j = NCH - 1
        i = l * NCH + j
        rc(m_all.at[j, cx, c], m_all.at[j, cx, 1 - c], sp(sem_mp, j), dev_p).wait()
        wait(cp_d(i))
        last_rows(lax.rem(i, ND), cx)

    @jax.named_scope("last_far")
    def last_far(l):
        j = NCH - 1
        i = l * NCH + j
        rc(m_all.at[j, 1 - cx, c], m_all.at[j, 1 - cx, 1 - c], sp(sem_mf, j), dev_p).wait()
        last_rows(lax.rem(i, ND), 1 - cx)

        @pl.when(i + ND < L * NCH)
        def _():
            start(cp_d(i + ND))

    @jax.named_scope("swap")
    def swap(l):
        rc(m_all.at[NCH - 1, cx, c], m_all.at[NCH - 1, cx, c], sp(sem_mq, NCH - 1), dev_q).wait_send()
        for g in (cx, 1 - cx):
            for n in range(2):
                yx(g, n).wait()
        hr = rows // 2
        for g in range(2):
            for n in range(2):
                rr, cc = slice(g * hr, (g + 1) * hr), slice(n * half, (n + 1) * half)
                upd = yx_s[g, n].astype(F32) + yx_r[g, n].astype(F32)
                h_b[rr, cc] = (h_b[rr, cc].astype(F32) + upd).astype(BF)

    lax.fori_loop(0, L, layer, 0)
    hout[...] = h_b[:, pl.ds(pl.multiple_of(y * half, half), half)]


def solution(mesh):
    row_spec = P("dp", ("x", "yz"))
    tile_in = P(None, "x", "yz")
    tile_out = P(None, "yz", "x")
    cache_spec = P(None, ("dp", "x", "yz"))
    len_spec = P(("dp", "x", "yz"))

    def device_step(hidden, norm_gain, w_q, w_kv, w_gate, w_up, w_o, w_down, k_cache, v_cache, seq_len):
        L, k_in, q_cols = w_q.shape
        rows = hidden.shape[0]
        half = hidden.shape[1]
        kv_cols = w_kv.shape[2]
        ff = w_gate.shape[2]
        ch = CH
        nch = ff // ch
        d_out = w_o.shape[2]
        ns, cache_len, hd = k_cache.shape[1:]
        zc = q_cols + kv_cols
        dims = {"layers": L, "n_chunks": nch, "d": half * 8}
        vm = pl.BlockSpec(memory_space=pltpu.VMEM)
        anyspec = pl.BlockSpec(memory_space=pl.ANY)
        DMA = pltpu.SemaphoreType.DMA
        V = pltpu.VMEM
        h_new, k_new, v_new = pl.pallas_call(
            functools.partial(step_kernel, dims),
            out_shape=(
                jax.ShapeDtypeStruct(hidden.shape, BF),
                jax.ShapeDtypeStruct((L, ns, hd), BF),
                jax.ShapeDtypeStruct((L, ns, hd), BF),
            ),
            in_specs=[vm, vm] + [anyspec] * 8 + [pl.BlockSpec(memory_space=pltpu.SMEM)],
            out_specs=(vm, vm, vm),
            scratch_shapes=[
                V((k_in, q_cols), BF), V((k_in, kv_cols), BF),
                V((NG, k_in, ch), BF), V((NG, k_in, ch), BF),
                V((q_cols, d_out), BF), V((ND, ch, d_out), BF),
                V((ns, cache_len, hd), BF), V((ns, cache_len, hd), BF),
                V((2, rows, half), BF), V((rows, d_out), BF), V((rows, d_out), BF), V((2, rows // 2, d_out), F32),
                V((8, 128), F32), V((3, 8, 128), F32),
                V((nch, 2, 2, 16, 2 * ch), BF), V((nch, 2, 16, 2 * ch), BF), V((nch, 16, 2 * ch), BF),
                V((nch, 2, 2, 16, ch), BF),
                V((2, 2, 16, zc), BF), V((2, 16, zc), BF), V((16, zc), BF),
                V((2, ns, zc), BF), V((2, ns, zc), BF),
                V((2, ns, q_cols), BF), V((2, 2, 2, ns, q_cols), BF),
                V((2, 2, rows // 2, half), BF), V((2, 2, rows // 2, half), BF),
                DMA, DMA, DMA((NG,)), DMA((NG,)), DMA, DMA((ND,)), DMA, DMA,
                DMA((2,)), DMA((2, 3)), DMA((2, nch + 1)), DMA((2, nch + 1)),
                DMA((2, nch)), DMA((2, nch)), DMA((2, nch)),
                DMA((2,)), DMA((2,)), DMA((2,)), DMA((2,)), DMA((2,)), DMA((2, 2, 2)),
            ],
            compiler_params=pltpu.CompilerParams(
                collective_id=0, has_side_effects=True, vmem_limit_bytes=67_000_000),
            name="decode_step",
        )(hidden, norm_gain, w_q, w_kv, w_gate, w_up, w_o, w_down, k_cache, v_cache, seq_len)
        slot_hit = (jnp.arange(cache_len)[None, :] == seq_len[:, None])[None, :, :, None]
        k_out = jnp.where(slot_hit, k_new[:, :, None, :], k_cache)
        v_out = jnp.where(slot_hit, v_new[:, :, None, :], v_cache)
        return h_new, k_out, v_out

    return jax.shard_map(
        device_step,
        mesh=mesh,
        in_specs=(row_spec, P(None, "x"), tile_in, tile_in, tile_in, tile_in, tile_out, tile_out, cache_spec, cache_spec, len_spec),
        out_specs=(row_spec, cache_spec, cache_spec),
        check_vma=False,
    )
```

```python
import functools

import jax
import jax.numpy as jnp
from jax import lax
from jax.experimental import pallas as pl
from jax.experimental.pallas import tpu as pltpu
from jax.sharding import PartitionSpec as P

NORM_EPS = 1e-6
MESH = pl.DeviceIdType.MESH
BF = jnp.bfloat16
F32 = jnp.float32

CH = 1024
NG = 7
ND = 8
T_B = (1, 2, 3, 4, 5, 6, 7, 8)
T_C = (4, 6, 8, 9, 10, 11, 12, 14)
T_D = (10, 12, 15, 16, 17, 18, 19)
T_EN = (8, 9, 10, 11, 12, 13, 14)
T_EF = (12, 14, 17, 18, 19, 20, 21)
T_QB, T_QC, T_ATT, T_OS, T_ON, T_OF, T_OE, T_LN = 0, 2, 5, 8, 10, 14, 16, 15
STEPS = 22


def step_kernel(dims, hid, gain, wq, wkv, wg, wu, wo, wd, kc, vc, lens,
                hout, knew, vnew,
                wq_b, wkv_b, wg_b, wu_b, wo_b, wd_b, k_b, v_b,
                hin, h_b, u_b, acc, ss_s, ss_r, ss0, tot,
                part, rb, ib, m_all, part_q, rb_q, ib_q, zq, yq, ob, o_all, yx_s, yx_r,
                sem_wq, sem_wkv, sem_g, sem_u, sem_wo, sem_d, sem_k, sem_v,
                sem_h, sem_s0, sem_ss, sem_rb, sem_ib, sem_mp, sem_mq, sem_mf,
                sem_zq, sem_oy, sem_op, sem_oq, sem_of, sem_yx):
    L, NCH, D = dims["layers"], dims["n_chunks"], dims["d"]
    HD = 256
    QC = wq_b.shape[1]
    x = lax.axis_index("x")
    y = lax.axis_index("yz")
    c = lax.rem(x, 2)
    cx = x // 2
    xp = x + 1 - 2 * c
    xq = lax.rem(x + 2, 4)
    xd = 3 - x
    dev_p, dev_q, dev_d, dev_y = {"x": xp}, {"x": xq}, {"x": xd}, {"yz": 1 - y}

    def rc(src, dst, sems, dev):
        return pltpu.make_async_remote_copy(
            src_ref=src, dst_ref=dst, send_sem=sems[0], recv_sem=sems[1],
            device_id=dev, device_id_type=MESH)

    def sp(s, *idx):
        return (s.at[(0,) + idx], s.at[(1,) + idx])

    def cp_q(l):
        return (pltpu.make_async_copy(wq.at[l], wq_b, sem_wq),
                pltpu.make_async_copy(wkv.at[l], wkv_b, sem_wkv))

    def cp_gu(i):
        l, j, s = i // NCH, lax.rem(i, NCH), lax.rem(i, NG)
        cols = pl.ds(pl.multiple_of(j * CH, CH), CH)
        return (pltpu.make_async_copy(wg.at[l, :, cols], wg_b.at[s], sem_g.at[s]),
                pltpu.make_async_copy(wu.at[l, :, cols], wu_b.at[s], sem_u.at[s]))

    def cp_d(i):
        l, j, s = i // NCH, lax.rem(i, NCH), lax.rem(i, ND)
        rows = pl.ds(pl.multiple_of(j * CH, CH), CH)
        return (pltpu.make_async_copy(wd.at[l, rows, :], wd_b.at[s], sem_d.at[s]),)

    def cp_o(l):
        return (pltpu.make_async_copy(wo.at[l], wo_b, sem_wo),)

    def cp_kv(l):
        return (pltpu.make_async_copy(kc.at[l], k_b, sem_k),
                pltpu.make_async_copy(vc.at[l], v_b, sem_v))

    def start(cs):
        for cpy in cs:
            cpy.start()

    def wait(cs):
        for cpy in cs:
            cpy.wait()

    start(cp_q(0))
    for k in range(4):
        start(cp_gu(k))

    rows = hid.shape[0]
    eye = (lax.broadcasted_iota(jnp.int32, (rows, 128), 0)
           == lax.broadcasted_iota(jnp.int32, (rows, 128), 1))

    def row_sums(h):
        ss = jnp.sum(h * h, axis=1, keepdims=True)
        row = jnp.sum(jnp.where(eye, ss, 0.0), axis=0, keepdims=True)
        return jnp.broadcast_to(row, tot.shape)

    me = x * 2 + y
    ss0[me] = row_sums(hid[...].astype(F32))

    def other(k):
        return {"x": lax.rem(x + k // 2, 4), "yz": lax.rem(y + k % 2, 2)}

    with jax.named_scope("barrier"):
        barrier = pltpu.get_barrier_semaphore()
        for k in range(1, 8):
            pl.semaphore_signal(barrier, inc=1, device_id=other(k), device_id_type=MESH)
        pl.semaphore_wait(barrier, 7)

    with jax.named_scope("hx"):
        h_send = rc(hid, hin.at[y], sp(sem_h), dev_y)
        h_send.start()
        s0 = [rc(ss0.at[me], ss0.at[me], sp(sem_s0, k), other(k)) for k in range(1, 8)]
        for cpy in s0:
            cpy.start()
        for k in range(4, NG):
            start(cp_gu(k))
        start(cp_kv(0))
        hin[y] = hid[...]
        rc(hid, hin.at[1 - y], sp(sem_h), dev_y).wait_recv()
        half = hid.shape[1]
        h_b[:, :half] = hin[0]
        h_b[:, half:] = hin[1]
        h_send.wait_send()
        for cpy in s0:
            cpy.wait_send()
        for k in range(1, 8):
            frm = lax.rem(x + 4 - k // 2, 4) * 2 + lax.rem(y + 2 - k % 2, 2)
            rc(ss0.at[frm], ss0.at[frm], sp(sem_s0, k), other(k)).wait_recv()
        total = ss0[0]
        for k in range(1, 8):
            total = total + ss0[k]
        tot[...] = total

    def norm_exchange():
        ss_s[...] = row_sums(h_b[...].astype(F32))
        cps = [rc(ss_s, ss_r.at[k], sp(sem_ss, k), dev)
               for k, dev in enumerate((dev_p, dev_q, dev_d))]
        for cpy in cps:
            cpy.start()
        for cpy in cps:
            cpy.wait()
        tot[...] = (ss_s[...] + ss_r[0]) + (ss_r[1] + ss_r[2])

    @jax.named_scope("norm")
    def norm(l):
        pl.when(l > 0)(norm_exchange)
        gall = gain[...].astype(F32)
        g = gall[0:1]
        for k in range(1, L):
            g = jnp.where(l == k, gall[k:k + 1], g)
        tot_col = jnp.sum(jnp.where(eye, jnp.broadcast_to(tot[0:1], eye.shape), 0.0), axis=1, keepdims=True)
        inv = lax.rsqrt(tot_col / D + NORM_EPS)
        u_b[...] = (h_b[...].astype(F32) * inv * g).astype(BF)

    def put_rows(dst, cols, val):
        v = val.astype(BF)
        for r in range(4):
            dst[r // 2, r % 2, :, cols] = v[16 * r:16 * r + 16]

    pieces = (slice(0, QC // 2), slice(QC // 2, QC + HD))

    def to_p_q(k):
        cols = pieces[k]
        return rc(part_q.at[:, 1 - c, :, cols], rb_q.at[:, :, cols], sp(sem_rb, NCH + k), dev_p)

    def to_q_q(k):
        cols = pieces[k]
        return rc(part_q.at[1 - cx, c, :, cols], ib_q.at[:, cols], sp(sem_ib, NCH + k), dev_q)

    @jax.named_scope("a_q")
    def a_q(l):
        wait(cp_q(l))
        u = u_b[...]
        for k in range(2):
            for n in range(k * QC // 2, (k + 1) * QC // 2, 512):
                put_rows(part_q, slice(n, n + 512), jnp.dot(u, wq_b[:, n:n + 512], preferred_element_type=F32))
            if k == 1:
                put_rows(part_q, slice(QC, QC + HD), jnp.dot(u, wkv_b[...], preferred_element_type=F32))
            to_p_q(k).start()

        @pl.when(l + 1 < L)
        def _():
            start(cp_q(l + 1))

    @jax.named_scope("b_q")
    def b_q(k):
        cols = pieces[k]
        to_p_q(k).wait()
        s = part_q[1 - cx, c, :, cols].astype(F32) + rb_q[1 - cx, :, cols].astype(F32)
        part_q[1 - cx, c, :, cols] = s.astype(BF)
        to_q_q(k).start()

    @jax.named_scope("c_q")
    def c_q():
        for k in range(2):
            to_q_q(k).wait()
        z = (part_q[cx, c].astype(F32) + rb_q[cx].astype(F32)) + ib_q[...].astype(F32)
        zq[0] = z[0:8].astype(BF)
        zq[1] = z[8:16].astype(BF)
        rc(zq.at[1 - y], yq.at[y], sp(sem_zq), dev_y).start()
        yq[y] = zq[y]

    @jax.named_scope("attend")
    def attend(l):
        rc(zq.at[1 - y], yq.at[1 - y], sp(sem_zq), dev_y).wait()
        q0 = yq[0].astype(F32)
        q1 = yq[1].astype(F32)
        k_new = q0[:, QC:]
        v_new = q1[:, QC:]
        knew[l] = k_new.astype(BF)
        vnew[l] = v_new.astype(BF)
        nh = QC // HD
        ns = 8
        heads = [qq[:, h * HD:(h + 1) * HD] for qq in (q0, q1) for h in range(nh)]
        qf = jnp.concatenate(heads, axis=0)
        qb = qf.astype(BF)
        nr = 2 * nh * ns
        pos = lax.broadcasted_iota(jnp.int32, (nr, HD), 1)
        seq = lax.rem(lax.broadcasted_iota(jnp.int32, (nr, HD), 0), ns)
        ln = jnp.zeros((nr, HD), jnp.int32)
        for b in range(ns):
            ln = jnp.where(seq == b, lens[b], ln)
        k_rep = jnp.concatenate([k_new] * (2 * nh), axis=0)
        v_rep = jnp.concatenate([v_new] * (2 * nh), axis=0)
        s_new = jnp.sum(qf * k_rep, axis=1, keepdims=True)
        wait(cp_kv(l))
        s = jnp.zeros((nr, HD), F32)
        for b in range(ns):
            sb = lax.dot_general(qb, k_b[b], (((1,), (1,)), ((), ())), preferred_element_type=F32)
            s = jnp.where(seq == b, sb, s)
        s = jnp.where(pos == ln, s_new, s) * HD ** -0.5
        s = jnp.where(pos <= ln, s, -1e30)
        e = jnp.exp(s - jnp.max(s, axis=1, keepdims=True))
        p = (e / jnp.sum(e, axis=1, keepdims=True)).astype(BF).astype(F32)
        p_new = jnp.sum(jnp.where(pos == ln, p, 0.0), axis=1, keepdims=True)
        p_old = jnp.where(pos == ln, 0.0, p)
        o = p_new * v_rep
        for b in range(ns):
            pb = jnp.where(seq == b, p_old, 0.0).astype(BF)
            o = o + jnp.dot(pb, v_b[b], preferred_element_type=F32)
        for hh in range(2):
            for h in range(nh):
                r0 = (hh * nh + h) * ns
                ob[hh, :, h * HD:(h + 1) * HD] = o[r0:r0 + ns].astype(BF)
        rc(ob.at[1 - y], o_all.at[cx, c, y], sp(sem_oy), dev_y).start()
        o_all[cx, c, y] = ob[y]

        @pl.when(l + 1 < L)
        def _():
            start(cp_kv(l + 1))

    @jax.named_scope("o_send")
    def o_send():
        rc(ob.at[1 - y], o_all.at[cx, c, 1 - y], sp(sem_oy), dev_y).wait()
        rc(o_all.at[cx, c], o_all.at[cx, c], sp(sem_op), dev_p).start()
        rc(o_all.at[cx, c], o_all.at[cx, c], sp(sem_oq), dev_q).start()

    @jax.named_scope("o_fwd")
    def o_fwd():
        rc(o_all.at[1 - cx, c], o_all.at[1 - cx, c], sp(sem_oq), dev_q).wait_recv()
        rc(o_all.at[1 - cx, c], o_all.at[1 - cx, c], sp(sem_of), dev_p).start()

    def o_rows(g):
        blocks = [o_all[g, i // 2, i % 2].astype(F32) for i in range(4)]
        lhs = jnp.concatenate(blocks, axis=0).astype(BF)
        for n in range(0, acc.shape[2], 512):
            acc[g, :, n:n + 512] += jnp.dot(lhs, wo_b[:, n:n + 512], preferred_element_type=F32)

    @jax.named_scope("o_near")
    def o_near(l):
        rc(o_all.at[cx, c], o_all.at[cx, 1 - c], sp(sem_op), dev_p).wait()
        wait(cp_o(l))
        o_rows(cx)

    @jax.named_scope("o_far")
    def o_far(l):
        rc(o_all.at[1 - cx, c], o_all.at[1 - cx, 1 - c], sp(sem_of), dev_p).wait()
        rc(o_all.at[cx, c], o_all.at[cx, c], sp(sem_oq), dev_q).wait_send()
        o_rows(1 - cx)

        @pl.when(l + 1 < L)
        def _():
            start(cp_o(l + 1))

    @jax.named_scope("stage_a")
    def stage_a(l, j):
        i = l * NCH + j
        s = lax.rem(i, NG)
        wait(cp_gu(i))
        u = u_b[...]
        dst = part.at[j]
        for n in range(0, CH, 512):
            put_rows(dst, slice(n, n + 512), jnp.dot(u, wg_b[s, :, n:n + 512], preferred_element_type=F32))
            put_rows(dst, slice(CH + n, CH + n + 512), jnp.dot(u, wu_b[s, :, n:n + 512], preferred_element_type=F32))
        rc(part.at[j, :, 1 - c], rb.at[j], sp(sem_rb, j), dev_p).start()

        @pl.when(i + NG < L * NCH)
        def _():
            start(cp_gu(i + NG))

    @jax.named_scope("stage_b")
    def stage_b(j):
        rc(part.at[j, :, 1 - c], rb.at[j], sp(sem_rb, j), dev_p).wait()
        s = part[j, 1 - cx, c].astype(F32) + rb[j, 1 - cx].astype(F32)
        part[j, 1 - cx, c] = s.astype(BF)
        rc(part.at[j, 1 - cx, c], ib.at[j], sp(sem_ib, j), dev_q).start()

    @jax.named_scope("stage_c")
    def stage_c(j):
        rc(part.at[j, 1 - cx, c], ib.at[j], sp(sem_ib, j), dev_q).wait()
        z = (part[j, cx, c].astype(F32) + rb[j, cx].astype(F32)) + ib[j].astype(F32)
        z = z.astype(BF).astype(F32)
        gate, up = z[:, :CH], z[:, CH:]
        m_all[j, cx, c] = (jax.nn.silu(gate) * up).astype(BF)
        rc(m_all.at[j, cx, c], m_all.at[j, cx, c], sp(sem_mq, j), dev_q).start()

        @pl.when(j == NCH - 1)
        def _():
            rc(m_all.at[j, cx, c], m_all.at[j, cx, c], sp(sem_mf, j), dev_d).start()

        rc(m_all.at[j, cx, c], m_all.at[j, cx, c], sp(sem_mp, j), dev_p).start()

    @jax.named_scope("stage_d")
    def stage_d(j):
        rc(m_all.at[j, 1 - cx, c], m_all.at[j, 1 - cx, c], sp(sem_mq, j), dev_q).wait_recv()
        rc(m_all.at[j, 1 - cx, c], m_all.at[j, 1 - cx, c], sp(sem_mf, j), dev_p).start()

    def e_rows(s, j, g):
        m = m_all[j, g].reshape(rows // 2, CH)
        for n in range(0, acc.shape[2], 512):
            acc[g, :, n:n + 512] += jnp.dot(m, wd_b[s, :, n:n + 512], preferred_element_type=F32)

    @jax.named_scope("e_near")
    def e_near(l, j):
        i = l * NCH + j
        rc(m_all.at[j, cx, c], m_all.at[j, cx, 1 - c], sp(sem_mp, j), dev_p).wait()
        wait(cp_d(i))
        e_rows(lax.rem(i, ND), j, cx)

    @jax.named_scope("e_far")
    def e_far(l, j):
        i = l * NCH + j
        rc(m_all.at[j, 1 - cx, c], m_all.at[j, 1 - cx, 1 - c], sp(sem_mf, j), dev_p).wait()
        rc(m_all.at[j, cx, c], m_all.at[j, cx, c], sp(sem_mq, j), dev_q).wait_send()
        e_rows(lax.rem(i, ND), j, 1 - cx)

        @pl.when(i + ND < L * NCH)
        def _():
            start(cp_d(i + ND))

    def layer(l, carry):
        norm(l)
        acc[...] = jnp.zeros_like(acc)
        a_q(l)
        b_q(0)

        def step(t, carry2):
            def at(steps, fn):
                if isinstance(steps, int):
                    pl.when(t == steps)(fn)
                    return
                hit = t == steps[0]
                j = jnp.int32(0)
                for k, st in enumerate(steps[1:]):
                    hit = hit | (t == st)
                    j = jnp.where(t >= st, k + 1, j)
                pl.when(hit)(lambda: fn(j))

            pl.when(t < NCH)(lambda: stage_a(l, t))
            pl.when((l == 0) & (t < ND))(lambda: start(cp_d(t)))
            pl.when((l == 0) & (t == 3))(lambda: start(cp_o(0)))
            at(T_QB, lambda: b_q(1))
            at(T_B, stage_b)
            at(T_QC, c_q)
            at(T_OS, o_send)
            at(T_LN, lambda: last_near(l))
            at(T_D, stage_d)
            at(T_EN, lambda j: e_near(l, j))
            at(T_ON, lambda: o_near(l))
            at(T_OE, lambda: o_far(l))
            at(T_EF, lambda j: e_far(l, j))
            at(T_C, stage_c)
            at(T_OF, o_fwd)
            at(T_ATT, lambda: attend(l))
            return carry2

        lax.fori_loop(0, STEPS, step, 0)

        last_far(l)
        swap(l)
        return carry

    def yx(g, n):
        return rc(yx_s.at[g, n], yx_r.at[g, n], sp(sem_yx, g, n), dev_y)

    def last_rows(l, s, g):
        m = m_all[NCH - 1, g].reshape(rows // 2, CH)
        for n in (1 - y, y):
            cols = pl.ds(pl.multiple_of(n * half, half), half)
            v = acc[g, :, cols] + jnp.dot(m, wd_b[s, :, cols], preferred_element_type=F32)
            yx_s[g, n] = v.astype(BF)
            if n is y:
                pl.when(l + 1 < L)(lambda: yx(g, y).start())
            else:
                yx(g, n).start()

    @jax.named_scope("last_near")
    def last_near(l):
        j = NCH - 1
        i = l * NCH + j
        rc(m_all.at[j, cx, c], m_all.at[j, cx, 1 - c], sp(sem_mp, j), dev_p).wait()
        wait(cp_d(i))
        last_rows(l, lax.rem(i, ND), cx)

    @jax.named_scope("last_far")
    def last_far(l):
        j = NCH - 1
        i = l * NCH + j
        rc(m_all.at[j, cx, c], m_all.at[j, 1 - cx, c], sp(sem_mq, j), dev_q).wait_recv()
        rc(m_all.at[j, cx, c], m_all.at[j, 1 - cx, 1 - c], sp(sem_mf, j), dev_d).wait_recv()
        last_rows(l, lax.rem(i, ND), 1 - cx)

        @pl.when(i + ND < L * NCH)
        def _():
            start(cp_d(i + ND))

    @jax.named_scope("swap")
    def swap(l):
        rc(m_all.at[NCH - 1, cx, c], m_all.at[NCH - 1, cx, c], sp(sem_mq, NCH - 1), dev_q).wait_send()
        rc(m_all.at[NCH - 1, cx, c], m_all.at[NCH - 1, cx, c], sp(sem_mf, NCH - 1), dev_d).wait_send()
        for g in (cx, 1 - cx):
            yx(g, y).wait_recv()
            yx(g, 1 - y).wait_send()

        @pl.when(l + 1 < L)
        def _():
            for g in (cx, 1 - cx):
                yx(g, 1 - y).wait_recv()
                yx(g, y).wait_send()

        hr = rows // 2
        for g in range(2):
            for n in range(2):
                rr, cc = slice(g * hr, (g + 1) * hr), slice(n * half, (n + 1) * half)
                upd = yx_s[g, n].astype(F32) + yx_r[g, n].astype(F32)
                h_b[rr, cc] = (h_b[rr, cc].astype(F32) + upd).astype(BF)

    lax.fori_loop(0, L, layer, 0)
    hout[...] = h_b[:, pl.ds(pl.multiple_of(y * half, half), half)]


def place_kernel(kn, vn, hn, kc, vc, lens, ko, vo, ho, new_b, h_b, kv_b, sem_n, sem_h, sem_in, sem_out):
    L, ns, _, hd = kc.shape
    T = 16
    pairs = [(a, l) for l in range(L) for a in range(2)]
    news = [pltpu.make_async_copy((kn, vn)[a], new_b.at[a], sem_n.at[a]) for a in range(2)]
    h_in = pltpu.make_async_copy(hn, h_b, sem_h)
    ins = [pltpu.make_async_copy((kc, vc)[a].at[l], kv_b.at[a, l], sem_in.at[a, l]) for a, l in pairs]
    outs = [pltpu.make_async_copy(kv_b.at[a, l], (ko, vo)[a].at[l], sem_out.at[a, l]) for a, l in pairs]
    for cpy in news + ins + [h_in]:
        cpy.start()
    for cpy in news:
        cpy.wait()
    row = lax.broadcasted_iota(jnp.int32, (T, hd), 0)
    for k, (a, l) in enumerate(pairs):
        ins[k].wait()
        for b in range(ns):
            base = pl.multiple_of(lens[b] // T * T, T)
            tile = kv_b[a, l, b, pl.ds(base, T), :].astype(F32)
            new = new_b[a, l, b:b + 1, :].astype(F32)
            kv_b[a, l, b, pl.ds(base, T), :] = jnp.where(row == lens[b] - base, new, tile).astype(BF)
        outs[k].start()
    h_in.wait()
    h_out = pltpu.make_async_copy(h_b, ho, sem_h)
    h_out.start()
    for cpy in outs + [h_out]:
        cpy.wait()


def solution(mesh):
    row_spec = P("dp", ("x", "yz"))
    tile_in = P(None, "x", "yz")
    tile_out = P(None, "yz", "x")
    cache_spec = P(None, ("dp", "x", "yz"))
    len_spec = P(("dp", "x", "yz"))

    def device_step(hidden, norm_gain, w_q, w_kv, w_gate, w_up, w_o, w_down, k_cache, v_cache, seq_len):
        L, k_in, q_cols = w_q.shape
        rows = hidden.shape[0]
        half = hidden.shape[1]
        kv_cols = w_kv.shape[2]
        ff = w_gate.shape[2]
        ch = CH
        nch = ff // ch
        d_out = w_o.shape[2]
        ns, cache_len, hd = k_cache.shape[1:]
        zc = q_cols + kv_cols
        dims = {"layers": L, "n_chunks": nch, "d": half * 8}
        vm = pl.BlockSpec(memory_space=pltpu.VMEM)
        anyspec = pl.BlockSpec(memory_space=pl.ANY)
        DMA = pltpu.SemaphoreType.DMA
        V = pltpu.VMEM
        h_new, k_new, v_new = pl.pallas_call(
            functools.partial(step_kernel, dims),
            out_shape=(
                jax.ShapeDtypeStruct(hidden.shape, BF),
                jax.ShapeDtypeStruct((L, ns, hd), BF),
                jax.ShapeDtypeStruct((L, ns, hd), BF),
            ),
            in_specs=[vm, vm] + [anyspec] * 8 + [pl.BlockSpec(memory_space=pltpu.SMEM)],
            out_specs=(vm, vm, vm),
            scratch_shapes=[
                V((k_in, q_cols), BF), V((k_in, kv_cols), BF),
                V((NG, k_in, ch), BF), V((NG, k_in, ch), BF),
                V((q_cols, d_out), BF), V((ND, ch, d_out), BF),
                V((ns, cache_len, hd), BF), V((ns, cache_len, hd), BF),
                V((2, rows, half), BF), V((rows, d_out), BF), V((rows, d_out), BF), V((2, rows // 2, d_out), F32),
                V((8, 128), F32), V((3, 8, 128), F32), V((8, 8, 128), F32), V((8, 128), F32),
                V((nch, 2, 2, 16, 2 * ch), BF), V((nch, 2, 16, 2 * ch), BF), V((nch, 16, 2 * ch), BF),
                V((nch, 2, 2, 16, ch), BF),
                V((2, 2, 16, zc), BF), V((2, 16, zc), BF), V((16, zc), BF),
                V((2, ns, zc), BF), V((2, ns, zc), BF),
                V((2, ns, q_cols), BF), V((2, 2, 2, ns, q_cols), BF),
                V((2, 2, rows // 2, half), BF), V((2, 2, rows // 2, half), BF),
                DMA, DMA, DMA((NG,)), DMA((NG,)), DMA, DMA((ND,)), DMA, DMA,
                DMA((2,)), DMA((2, 8)), DMA((2, 3)), DMA((2, nch + 2)), DMA((2, nch + 2)),
                DMA((2, nch)), DMA((2, nch)), DMA((2, nch)),
                DMA((2,)), DMA((2,)), DMA((2,)), DMA((2,)), DMA((2,)), DMA((2, 2, 2)),
            ],
            compiler_params=pltpu.CompilerParams(
                collective_id=0, has_side_effects=True, vmem_limit_bytes=67_000_000),
            name="decode_step",
        )(hidden, norm_gain, w_q, w_kv, w_gate, w_up, w_o, w_down, k_cache, v_cache, seq_len)
        k_out, v_out, h_out = pl.pallas_call(
            place_kernel,
            out_shape=(
                jax.ShapeDtypeStruct(k_cache.shape, BF),
                jax.ShapeDtypeStruct(v_cache.shape, BF),
                jax.ShapeDtypeStruct(hidden.shape, BF),
            ),
            in_specs=[anyspec] * 5 + [pl.BlockSpec(memory_space=pltpu.SMEM)],
            out_specs=(anyspec,) * 3,
            scratch_shapes=[
                V((2, L, ns, hd), BF), V((rows, half), BF), V((2, L, ns, cache_len, hd), BF),
                DMA((2,)), DMA, DMA((2, L)), DMA((2, L)),
            ],
            compiler_params=pltpu.CompilerParams(vmem_limit_bytes=60_000_000),
            name="place_rows",
        )(k_new, v_new, h_new, k_cache, v_cache, seq_len)
        return h_out, k_out, v_out

    return jax.shard_map(
        device_step,
        mesh=mesh,
        in_specs=(row_spec, P(None, "x"), tile_in, tile_in, tile_in, tile_in, tile_out, tile_out, cache_spec, cache_spec, len_spec),
        out_specs=(row_spec, cache_spec, cache_spec),
        check_vma=False,
    )
```

```python
import functools

import jax
import jax.numpy as jnp
from jax import lax
from jax.experimental import pallas as pl
from jax.experimental.pallas import tpu as pltpu
from jax.sharding import PartitionSpec as P

NORM_EPS = 1e-6
SHRINK = 2.0 ** -64
MESH = pl.DeviceIdType.MESH
BF = jnp.bfloat16
F32 = jnp.float32

CH = 1024
NG = 7
ND = 8
T_B = (1, 2, 3, 4, 5, 6, 7, 8)
T_C = (4, 6, 8, 9, 10, 11, 12, 14)
T_D = (10, 12, 15, 16, 17, 18, 19)
T_EN = (8, 9, 10, 11, 12, 13, 14)
T_EF = (12, 14, 17, 18, 19, 20, 21)
T_QB, T_QC, T_ATT, T_OS, T_ON, T_OF, T_OE, T_LN = 0, 3, 6, 9, 11, 14, 16, 15
STEPS = 22


def step_kernel(dims, hid, gain, wq, wkv, wg, wu, wo, wd, kc, vc, lens,
                hout, knew, vnew,
                wq_b, wkv_b, wg_b, wu_b, wo_b, wd_b, k_b, v_b,
                hin, h_b, u_b, acc, ss_s, ss_r, ss0, tot, sc_b,
                part, rb, ib, m_all, part_q, rb_q, ib_q, zq, yq, ob, o_all, yx_s, yx_r,
                sem_wq, sem_wkv, sem_g, sem_u, sem_wo, sem_d, sem_k, sem_v,
                sem_h, sem_s0, sem_ss, sem_rb, sem_ib, sem_mp, sem_mq, sem_mf,
                sem_zq, sem_oy, sem_op, sem_oq, sem_of, sem_yx):
    L, NCH, D = dims["layers"], dims["n_chunks"], dims["d"]
    HD = 256
    QC = wq_b.shape[1]
    x = lax.axis_index("x")
    y = lax.axis_index("yz")
    c = lax.rem(x, 2)
    cx = x // 2
    xp = x + 1 - 2 * c
    xq = lax.rem(x + 2, 4)
    xd = 3 - x
    dev_p, dev_q, dev_d, dev_y = {"x": xp}, {"x": xq}, {"x": xd}, {"yz": 1 - y}

    def rc(src, dst, sems, dev):
        return pltpu.make_async_remote_copy(
            src_ref=src, dst_ref=dst, send_sem=sems[0], recv_sem=sems[1],
            device_id=dev, device_id_type=MESH)

    def sp(s, *idx):
        return (s.at[(0,) + idx], s.at[(1,) + idx])

    def cp_q(l):
        return (pltpu.make_async_copy(wq.at[l], wq_b, sem_wq),
                pltpu.make_async_copy(wkv.at[l], wkv_b, sem_wkv))

    def cp_gu(i):
        l, j, s = i // NCH, lax.rem(i, NCH), lax.rem(i, NG)
        cols = pl.ds(pl.multiple_of(j * CH, CH), CH)
        return (pltpu.make_async_copy(wg.at[l, :, cols], wg_b.at[s], sem_g.at[s]),
                pltpu.make_async_copy(wu.at[l, :, cols], wu_b.at[s], sem_u.at[s]))

    def cp_d(i):
        l, j, s = i // NCH, lax.rem(i, NCH), lax.rem(i, ND)
        rows = pl.ds(pl.multiple_of(j * CH, CH), CH)
        return (pltpu.make_async_copy(wd.at[l, rows, :], wd_b.at[s], sem_d.at[s]),)

    def cp_o(l):
        return (pltpu.make_async_copy(wo.at[l], wo_b, sem_wo),)

    def cp_kv(l):
        return (pltpu.make_async_copy(kc.at[l], k_b, sem_k),
                pltpu.make_async_copy(vc.at[l], v_b, sem_v))

    def start(cs):
        for cpy in cs:
            cpy.start()

    def wait(cs):
        for cpy in cs:
            cpy.wait()

    start(cp_q(0))
    for k in range(4):
        start(cp_gu(k))

    rows = hid.shape[0]
    eye = (lax.broadcasted_iota(jnp.int32, (rows, 128), 0)
           == lax.broadcasted_iota(jnp.int32, (rows, 128), 1))

    def row_sums(h):
        ss = jnp.sum(h * h, axis=1, keepdims=True)
        row = jnp.sum(jnp.where(eye, ss, 0.0), axis=0, keepdims=True)
        return jnp.broadcast_to(row, tot.shape)

    me = x * 2 + y
    ss0[me] = row_sums(hid[...].astype(F32))

    def other(k):
        return {"x": lax.rem(x + k // 2, 4), "yz": lax.rem(y + k % 2, 2)}

    with jax.named_scope("barrier"):
        barrier = pltpu.get_barrier_semaphore()
        for k in range(1, 8):
            pl.semaphore_signal(barrier, inc=1, device_id=other(k), device_id_type=MESH)
        pl.semaphore_wait(barrier, 7)

    with jax.named_scope("hx"):
        h_send = rc(hid, hin.at[y], sp(sem_h), dev_y)
        h_send.start()
        s0 = [rc(ss0.at[me], ss0.at[me], sp(sem_s0, k), other(k)) for k in range(1, 8)]
        for cpy in s0:
            cpy.start()
        for k in range(4, NG):
            start(cp_gu(k))
        start(cp_kv(0))
        hin[y] = hid[...]
        rc(hid, hin.at[1 - y], sp(sem_h), dev_y).wait_recv()
        half = hid.shape[1]
        h_b[:, :half] = hin[0]
        h_b[:, half:] = hin[1]
        h_send.wait_send()
        for cpy in s0:
            cpy.wait_send()
        for k in range(1, 8):
            frm = lax.rem(x + 4 - k // 2, 4) * 2 + lax.rem(y + 2 - k % 2, 2)
            rc(ss0.at[frm], ss0.at[frm], sp(sem_s0, k), other(k)).wait_recv()
        total = ss0[0]
        for k in range(1, 8):
            total = total + ss0[k]
        tot[...] = total

    def sums(k, dev):
        return rc(ss_s, ss_r.at[k], sp(sem_ss, k), dev)

    def send_sums():
        ss_s[...] = row_sums(h_b[...].astype(F32))
        for k, dev in enumerate((dev_p, dev_q, dev_d)):
            sums(k, dev).start()

    def get_sums():
        for k, dev in enumerate((dev_p, dev_q, dev_d)):
            sums(k, dev).wait()
        tot[...] = (ss_s[...] + ss_r[0]) + (ss_r[1] + ss_r[2])

    @jax.named_scope("norm")
    def norm(l):
        pl.when(l > 0)(send_sums)
        gall = gain[...].astype(F32)
        g = gall[0:1]
        for k in range(1, L):
            g = jnp.where(l == k, gall[k:k + 1], g)
        u_b[...] = (h_b[...].astype(F32) * (g * SHRINK)).astype(BF)

    @jax.named_scope("scale")
    def row_scale(l):
        pl.when(l > 0)(get_sums)
        tot_col = jnp.sum(jnp.where(eye, jnp.broadcast_to(tot[0:1], eye.shape), 0.0), axis=1, keepdims=True)
        sc = jnp.broadcast_to(lax.rsqrt(tot_col / D + NORM_EPS) / SHRINK, eye.shape)
        for r in range(4):
            sc_b[r // 2, r % 2] = sc[16 * r:16 * r + 16]

    def scaled(z):
        sc = sc_b[cx, c][:, 0:1]
        return jnp.where(sc > 0.0, z * sc, 0.0)

    def put_rows(dst, cols, val):
        v = val.astype(BF)
        for r in range(4):
            dst[r // 2, r % 2, :, cols] = v[16 * r:16 * r + 16]

    pieces = (slice(0, QC // 2), slice(QC // 2, QC + HD))

    def to_p_q(k):
        cols = pieces[k]
        return rc(part_q.at[:, 1 - c, :, cols], rb_q.at[:, :, cols], sp(sem_rb, NCH + k), dev_p)

    def to_q_q(k):
        cols = pieces[k]
        return rc(part_q.at[1 - cx, c, :, cols], ib_q.at[:, cols], sp(sem_ib, NCH + k), dev_q)

    @jax.named_scope("a_q")
    def a_q(l):
        wait(cp_q(l))
        u = u_b[...]
        for k in range(2):
            for n in range(k * QC // 2, (k + 1) * QC // 2, 512):
                put_rows(part_q, slice(n, n + 512), jnp.dot(u, wq_b[:, n:n + 512], preferred_element_type=F32))
            if k == 1:
                put_rows(part_q, slice(QC, QC + HD), jnp.dot(u, wkv_b[...], preferred_element_type=F32))
            to_p_q(k).start()

        @pl.when(l + 1 < L)
        def _():
            start(cp_q(l + 1))

    @jax.named_scope("b_q")
    def b_q(k):
        cols = pieces[k]
        to_p_q(k).wait()
        s = part_q[1 - cx, c, :, cols].astype(F32) + rb_q[1 - cx, :, cols].astype(F32)
        part_q[1 - cx, c, :, cols] = s.astype(BF)
        to_q_q(k).start()

    @jax.named_scope("c_q")
    def c_q(l):
        row_scale(l)
        for k in range(2):
            to_q_q(k).wait()
        z = scaled((part_q[cx, c].astype(F32) + rb_q[cx].astype(F32)) + ib_q[...].astype(F32))
        zq[0] = z[0:8].astype(BF)
        zq[1] = z[8:16].astype(BF)
        rc(zq.at[1 - y], yq.at[y], sp(sem_zq), dev_y).start()
        yq[y] = zq[y]

    @jax.named_scope("attend")
    def attend(l):
        rc(zq.at[1 - y], yq.at[1 - y], sp(sem_zq), dev_y).wait()
        q0 = yq[0].astype(F32)
        q1 = yq[1].astype(F32)
        k_new = q0[:, QC:]
        v_new = q1[:, QC:]
        knew[l] = k_new.astype(BF)
        vnew[l] = v_new.astype(BF)
        nh = QC // HD
        ns = 8
        heads = [qq[:, h * HD:(h + 1) * HD] for qq in (q0, q1) for h in range(nh)]
        qf = jnp.concatenate(heads, axis=0)
        qb = qf.astype(BF)
        nr = 2 * nh * ns
        pos = lax.broadcasted_iota(jnp.int32, (nr, HD), 1)
        seq = lax.rem(lax.broadcasted_iota(jnp.int32, (nr, HD), 0), ns)
        ln = jnp.zeros((nr, HD), jnp.int32)
        for b in range(ns):
            ln = jnp.where(seq == b, lens[b], ln)
        k_rep = jnp.concatenate([k_new] * (2 * nh), axis=0)
        v_rep = jnp.concatenate([v_new] * (2 * nh), axis=0)
        s_new = jnp.sum(qf * k_rep, axis=1, keepdims=True)
        wait(cp_kv(l))
        s = jnp.zeros((nr, HD), F32)
        for b in range(ns):
            sb = lax.dot_general(qb, k_b[b], (((1,), (1,)), ((), ())), preferred_element_type=F32)
            s = jnp.where(seq == b, sb, s)
        s = jnp.where(pos == ln, s_new, s) * HD ** -0.5
        s = jnp.where(pos <= ln, s, -1e30)
        e = jnp.exp(s - jnp.max(s, axis=1, keepdims=True))
        p = (e / jnp.sum(e, axis=1, keepdims=True)).astype(BF).astype(F32)
        p_new = jnp.sum(jnp.where(pos == ln, p, 0.0), axis=1, keepdims=True)
        p_old = jnp.where(pos == ln, 0.0, p)
        o = p_new * v_rep
        for b in range(ns):
            pb = jnp.where(seq == b, p_old, 0.0).astype(BF)
            o = o + jnp.dot(pb, v_b[b], preferred_element_type=F32)
        for hh in range(2):
            for h in range(nh):
                r0 = (hh * nh + h) * ns
                ob[hh, :, h * HD:(h + 1) * HD] = o[r0:r0 + ns].astype(BF)
        rc(ob.at[1 - y], o_all.at[cx, c, y], sp(sem_oy), dev_y).start()
        o_all[cx, c, y] = ob[y]

        @pl.when(l + 1 < L)
        def _():
            start(cp_kv(l + 1))

    @jax.named_scope("o_send")
    def o_send():
        rc(ob.at[1 - y], o_all.at[cx, c, 1 - y], sp(sem_oy), dev_y).wait()
        rc(o_all.at[cx, c], o_all.at[cx, c], sp(sem_op), dev_p).start()
        rc(o_all.at[cx, c], o_all.at[cx, c], sp(sem_oq), dev_q).start()

    @jax.named_scope("o_fwd")
    def o_fwd():
        rc(o_all.at[1 - cx, c], o_all.at[1 - cx, c], sp(sem_oq), dev_q).wait_recv()
        rc(o_all.at[1 - cx, c], o_all.at[1 - cx, c], sp(sem_of), dev_p).start()

    def o_rows(g):
        blocks = [o_all[g, i // 2, i % 2].astype(F32) for i in range(4)]
        lhs = jnp.concatenate(blocks, axis=0).astype(BF)
        for n in range(0, acc.shape[2], 512):
            acc[g, :, n:n + 512] += jnp.dot(lhs, wo_b[:, n:n + 512], preferred_element_type=F32)

    @jax.named_scope("o_near")
    def o_near(l):
        rc(o_all.at[cx, c], o_all.at[cx, 1 - c], sp(sem_op), dev_p).wait()
        wait(cp_o(l))
        o_rows(cx)

    @jax.named_scope("o_far")
    def o_far(l):
        rc(o_all.at[1 - cx, c], o_all.at[1 - cx, 1 - c], sp(sem_of), dev_p).wait()
        rc(o_all.at[cx, c], o_all.at[cx, c], sp(sem_oq), dev_q).wait_send()
        o_rows(1 - cx)

        @pl.when(l + 1 < L)
        def _():
            start(cp_o(l + 1))

    @jax.named_scope("stage_a")
    def stage_a(l, j):
        i = l * NCH + j
        s = lax.rem(i, NG)
        wait(cp_gu(i))
        u = u_b[...]
        dst = part.at[j]
        for n in range(0, CH, 512):
            put_rows(dst, slice(n, n + 512), jnp.dot(u, wg_b[s, :, n:n + 512], preferred_element_type=F32))
            put_rows(dst, slice(CH + n, CH + n + 512), jnp.dot(u, wu_b[s, :, n:n + 512], preferred_element_type=F32))
        rc(part.at[j, :, 1 - c], rb.at[j], sp(sem_rb, j), dev_p).start()

        @pl.when(i + NG < L * NCH)
        def _():
            start(cp_gu(i + NG))

    @jax.named_scope("stage_b")
    def stage_b(j):
        rc(part.at[j, :, 1 - c], rb.at[j], sp(sem_rb, j), dev_p).wait()
        s = part[j, 1 - cx, c].astype(F32) + rb[j, 1 - cx].astype(F32)
        part[j, 1 - cx, c] = s.astype(BF)
        rc(part.at[j, 1 - cx, c], ib.at[j], sp(sem_ib, j), dev_q).start()

    @jax.named_scope("stage_c")
    def stage_c(j):
        rc(part.at[j, 1 - cx, c], ib.at[j], sp(sem_ib, j), dev_q).wait()
        z = (part[j, cx, c].astype(F32) + rb[j, cx].astype(F32)) + ib[j].astype(F32)
        z = scaled(z).astype(BF).astype(F32)
        gate, up = z[:, :CH], z[:, CH:]
        m_all[j, cx, c] = (jax.nn.silu(gate) * up).astype(BF)
        rc(m_all.at[j, cx, c], m_all.at[j, cx, c], sp(sem_mq, j), dev_q).start()

        @pl.when(j == NCH - 1)
        def _():
            rc(m_all.at[j, cx, c], m_all.at[j, cx, c], sp(sem_mf, j), dev_d).start()

        rc(m_all.at[j, cx, c], m_all.at[j, cx, c], sp(sem_mp, j), dev_p).start()

    @jax.named_scope("stage_d")
    def stage_d(j):
        rc(m_all.at[j, 1 - cx, c], m_all.at[j, 1 - cx, c], sp(sem_mq, j), dev_q).wait_recv()
        rc(m_all.at[j, 1 - cx, c], m_all.at[j, 1 - cx, c], sp(sem_mf, j), dev_p).start()

    def e_rows(s, j, g):
        m = m_all[j, g].reshape(rows // 2, CH)
        for n in range(0, acc.shape[2], 512):
            acc[g, :, n:n + 512] += jnp.dot(m, wd_b[s, :, n:n + 512], preferred_element_type=F32)

    @jax.named_scope("e_near")
    def e_near(l, j):
        i = l * NCH + j
        rc(m_all.at[j, cx, c], m_all.at[j, cx, 1 - c], sp(sem_mp, j), dev_p).wait()
        wait(cp_d(i))
        e_rows(lax.rem(i, ND), j, cx)

    @jax.named_scope("e_far")
    def e_far(l, j):
        i = l * NCH + j
        rc(m_all.at[j, 1 - cx, c], m_all.at[j, 1 - cx, 1 - c], sp(sem_mf, j), dev_p).wait()
        rc(m_all.at[j, cx, c], m_all.at[j, cx, c], sp(sem_mq, j), dev_q).wait_send()
        e_rows(lax.rem(i, ND), j, 1 - cx)

        @pl.when(i + ND < L * NCH)
        def _():
            start(cp_d(i + ND))

    def layer(l, carry):
        norm(l)
        acc[...] = jnp.zeros_like(acc)
        a_q(l)
        b_q(0)

        def step(t, carry2):
            def at(steps, fn):
                if isinstance(steps, int):
                    pl.when(t == steps)(fn)
                    return
                hit = t == steps[0]
                j = jnp.int32(0)
                for k, st in enumerate(steps[1:]):
                    hit = hit | (t == st)
                    j = jnp.where(t >= st, k + 1, j)
                pl.when(hit)(lambda: fn(j))

            pl.when(t < NCH)(lambda: stage_a(l, t))
            pl.when((l == 0) & (t < ND))(lambda: start(cp_d(t)))
            pl.when((l == 0) & (t == 3))(lambda: start(cp_o(0)))
            at(T_QB, lambda: b_q(1))
            at(T_B, stage_b)
            at(T_QC, lambda: c_q(l))
            at(T_OS, o_send)
            at(T_LN, lambda: last_near(l))
            at(T_D, stage_d)
            at(T_EN, lambda j: e_near(l, j))
            at(T_ON, lambda: o_near(l))
            at(T_OE, lambda: o_far(l))
            at(T_EF, lambda j: e_far(l, j))
            at(T_C, stage_c)
            at(T_OF, o_fwd)
            at(T_ATT, lambda: attend(l))
            return carry2

        lax.fori_loop(0, STEPS, step, 0)

        last_far(l)
        swap(l)
        return carry

    def yx(g, n):
        return rc(yx_s.at[g, n], yx_r.at[g, n], sp(sem_yx, g, n), dev_y)

    def last_rows(l, s, g):
        m = m_all[NCH - 1, g].reshape(rows // 2, CH)
        for n in (1 - y, y):
            cols = pl.ds(pl.multiple_of(n * half, half), half)
            v = acc[g, :, cols] + jnp.dot(m, wd_b[s, :, cols], preferred_element_type=F32)
            yx_s[g, n] = v.astype(BF)
            if n is y:
                pl.when(l + 1 < L)(lambda: yx(g, y).start())
            else:
                yx(g, n).start()

    @jax.named_scope("last_near")
    def last_near(l):
        j = NCH - 1
        i = l * NCH + j
        rc(m_all.at[j, cx, c], m_all.at[j, cx, 1 - c], sp(sem_mp, j), dev_p).wait()
        wait(cp_d(i))
        last_rows(l, lax.rem(i, ND), cx)

    @jax.named_scope("last_far")
    def last_far(l):
        j = NCH - 1
        i = l * NCH + j
        rc(m_all.at[j, cx, c], m_all.at[j, 1 - cx, c], sp(sem_mq, j), dev_q).wait_recv()
        rc(m_all.at[j, cx, c], m_all.at[j, 1 - cx, 1 - c], sp(sem_mf, j), dev_d).wait_recv()
        last_rows(l, lax.rem(i, ND), 1 - cx)

        @pl.when(i + ND < L * NCH)
        def _():
            start(cp_d(i + ND))

    @jax.named_scope("swap")
    def swap(l):
        rc(m_all.at[NCH - 1, cx, c], m_all.at[NCH - 1, cx, c], sp(sem_mq, NCH - 1), dev_q).wait_send()
        rc(m_all.at[NCH - 1, cx, c], m_all.at[NCH - 1, cx, c], sp(sem_mf, NCH - 1), dev_d).wait_send()
        for g in (cx, 1 - cx):
            yx(g, y).wait_recv()
            yx(g, 1 - y).wait_send()

        @pl.when(l + 1 < L)
        def _():
            for g in (cx, 1 - cx):
                yx(g, 1 - y).wait_recv()
                yx(g, y).wait_send()

        hr = rows // 2
        for g in range(2):
            for n in range(2):
                rr, cc = slice(g * hr, (g + 1) * hr), slice(n * half, (n + 1) * half)
                upd = yx_s[g, n].astype(F32) + yx_r[g, n].astype(F32)
                h_b[rr, cc] = (h_b[rr, cc].astype(F32) + upd).astype(BF)

    lax.fori_loop(0, L, layer, 0)
    hout[...] = h_b[:, pl.ds(pl.multiple_of(y * half, half), half)]


def place_kernel(kn, vn, hn, kc, vc, lens, ko, vo, ho, new_b, h_b, kv_b, sem_n, sem_h, sem_in, sem_out):
    L, ns, _, hd = kc.shape
    T = 16
    pairs = [(a, l) for l in range(L) for a in range(2)]
    news = [pltpu.make_async_copy((kn, vn)[a], new_b.at[a], sem_n.at[a]) for a in range(2)]
    h_in = pltpu.make_async_copy(hn, h_b, sem_h)
    ins = [pltpu.make_async_copy((kc, vc)[a].at[l], kv_b.at[a, l], sem_in.at[a, l]) for a, l in pairs]
    outs = [pltpu.make_async_copy(kv_b.at[a, l], (ko, vo)[a].at[l], sem_out.at[a, l]) for a, l in pairs]
    for cpy in news + ins + [h_in]:
        cpy.start()
    for cpy in news:
        cpy.wait()
    row = lax.broadcasted_iota(jnp.int32, (T, hd), 0)
    for k, (a, l) in enumerate(pairs):
        ins[k].wait()
        for b in range(ns):
            base = pl.multiple_of(lens[b] // T * T, T)
            tile = kv_b[a, l, b, pl.ds(base, T), :].astype(F32)
            new = new_b[a, l, b:b + 1, :].astype(F32)
            kv_b[a, l, b, pl.ds(base, T), :] = jnp.where(row == lens[b] - base, new, tile).astype(BF)
        outs[k].start()
    h_in.wait()
    h_out = pltpu.make_async_copy(h_b, ho, sem_h)
    h_out.start()
    for cpy in outs + [h_out]:
        cpy.wait()


def solution(mesh):
    row_spec = P("dp", ("x", "yz"))
    tile_in = P(None, "x", "yz")
    tile_out = P(None, "yz", "x")
    cache_spec = P(None, ("dp", "x", "yz"))
    len_spec = P(("dp", "x", "yz"))

    def device_step(hidden, norm_gain, w_q, w_kv, w_gate, w_up, w_o, w_down, k_cache, v_cache, seq_len):
        L, k_in, q_cols = w_q.shape
        rows = hidden.shape[0]
        half = hidden.shape[1]
        kv_cols = w_kv.shape[2]
        ff = w_gate.shape[2]
        ch = CH
        nch = ff // ch
        d_out = w_o.shape[2]
        ns, cache_len, hd = k_cache.shape[1:]
        zc = q_cols + kv_cols
        dims = {"layers": L, "n_chunks": nch, "d": half * 8}
        vm = pl.BlockSpec(memory_space=pltpu.VMEM)
        anyspec = pl.BlockSpec(memory_space=pl.ANY)
        DMA = pltpu.SemaphoreType.DMA
        V = pltpu.VMEM
        h_new, k_new, v_new = pl.pallas_call(
            functools.partial(step_kernel, dims),
            out_shape=(
                jax.ShapeDtypeStruct(hidden.shape, BF),
                jax.ShapeDtypeStruct((L, ns, hd), BF),
                jax.ShapeDtypeStruct((L, ns, hd), BF),
            ),
            in_specs=[vm, vm] + [anyspec] * 8 + [pl.BlockSpec(memory_space=pltpu.SMEM)],
            out_specs=(vm, vm, vm),
            scratch_shapes=[
                V((k_in, q_cols), BF), V((k_in, kv_cols), BF),
                V((NG, k_in, ch), BF), V((NG, k_in, ch), BF),
                V((q_cols, d_out), BF), V((ND, ch, d_out), BF),
                V((ns, cache_len, hd), BF), V((ns, cache_len, hd), BF),
                V((2, rows, half), BF), V((rows, d_out), BF), V((rows, d_out), BF), V((2, rows // 2, d_out), F32),
                V((8, 128), F32), V((3, 8, 128), F32), V((8, 8, 128), F32), V((8, 128), F32), V((2, 2, 16, 128), F32),
                V((nch, 2, 2, 16, 2 * ch), BF), V((nch, 2, 16, 2 * ch), BF), V((nch, 16, 2 * ch), BF),
                V((nch, 2, 2, 16, ch), BF),
                V((2, 2, 16, zc), BF), V((2, 16, zc), BF), V((16, zc), BF),
                V((2, ns, zc), BF), V((2, ns, zc), BF),
                V((2, ns, q_cols), BF), V((2, 2, 2, ns, q_cols), BF),
                V((2, 2, rows // 2, half), BF), V((2, 2, rows // 2, half), BF),
                DMA, DMA, DMA((NG,)), DMA((NG,)), DMA, DMA((ND,)), DMA, DMA,
                DMA((2,)), DMA((2, 8)), DMA((2, 3)), DMA((2, nch + 2)), DMA((2, nch + 2)),
                DMA((2, nch)), DMA((2, nch)), DMA((2, nch)),
                DMA((2,)), DMA((2,)), DMA((2,)), DMA((2,)), DMA((2,)), DMA((2, 2, 2)),
            ],
            compiler_params=pltpu.CompilerParams(
                collective_id=0, has_side_effects=True, vmem_limit_bytes=67_000_000),
            name="decode_step",
        )(hidden, norm_gain, w_q, w_kv, w_gate, w_up, w_o, w_down, k_cache, v_cache, seq_len)
        k_out, v_out, h_out = pl.pallas_call(
            place_kernel,
            out_shape=(
                jax.ShapeDtypeStruct(k_cache.shape, BF),
                jax.ShapeDtypeStruct(v_cache.shape, BF),
                jax.ShapeDtypeStruct(hidden.shape, BF),
            ),
            in_specs=[anyspec] * 5 + [pl.BlockSpec(memory_space=pltpu.SMEM)],
            out_specs=(anyspec,) * 3,
            scratch_shapes=[
                V((2, L, ns, hd), BF), V((rows, half), BF), V((2, L, ns, cache_len, hd), BF),
                DMA((2,)), DMA, DMA((2, L)), DMA((2, L)),
            ],
            compiler_params=pltpu.CompilerParams(vmem_limit_bytes=60_000_000),
            name="place_rows",
        )(k_new, v_new, h_new, k_cache, v_cache, seq_len)
        return h_out, k_out, v_out

    return jax.shard_map(
        device_step,
        mesh=mesh,
        in_specs=(row_spec, P(None, "x"), tile_in, tile_in, tile_in, tile_in, tile_out, tile_out, cache_spec, cache_spec, len_spec),
        out_specs=(row_spec, cache_spec, cache_spec),
        check_vma=False,
    )
```

```python
import functools

import jax
import jax.numpy as jnp
from jax import lax
from jax.experimental import pallas as pl
from jax.experimental.pallas import tpu as pltpu
from jax.sharding import PartitionSpec as P

NORM_EPS = 1e-6
SHRINK = 2.0 ** -64
MESH = pl.DeviceIdType.MESH
BF = jnp.bfloat16
F32 = jnp.float32

CH = 1024
NG = 7
ND = 8
NE = 3
NF = 4
T_A = (0, 1, 5, 6, 7)
T_AL = (2, 3, 4)
T_B = (1, 2, 6, 7, 8)
C1, C2, C3 = 0, 5, 6
T_C1, T_C2, T_C3 = (4, 5, 6, 7, 8), (10,), (11, 13)
T_D = (9, 10, 11, 13, 14, 15, 16)
T_EA = (10, 11, 12, 14)
T_EN = (10, 12, 13)
T_EF = (16, 17, 18)
T_SC, T_QB, T_QC, T_ATT, T_OS, T_OF, T_OE, T_LN = 4, 0, 4, 7, 10, 14, 15, 15
STEPS = 19


def step_kernel(dims, hid, gain, wq, wkv, wg, wu, wo, wd, kc, vc, lens,
                hout, knew, vnew,
                wq_b, wkv_b, wg_b, wu_b, wo_b, wd_b, k_b, v_b,
                hin, h_b, u_b, acc, ss_s, ss_r, ss0, tot, sc_b,
                part, rb, ib, m_all, part_q, rb_q, ib_q, zq, yq, ob, o_all, yx_s, yx_r,
                sem_wq, sem_wkv, sem_g, sem_u, sem_wo, sem_d, sem_k, sem_v,
                sem_h, sem_s0, sem_ss, sem_rb, sem_ib, sem_mp, sem_mq, sem_mf,
                sem_zq, sem_oy, sem_op, sem_oq, sem_of, sem_yx):
    L, NCH, D = dims["layers"], dims["n_chunks"], dims["d"]
    HD = 256
    QC = wq_b.shape[1]
    x = lax.axis_index("x")
    y = lax.axis_index("yz")
    c = lax.rem(x, 2)
    cx = x // 2
    xp = x + 1 - 2 * c
    xq = lax.rem(x + 2, 4)
    xd = 3 - x
    dev_p, dev_q, dev_d, dev_y = {"x": xp}, {"x": xq}, {"x": xd}, {"yz": 1 - y}

    def rc(src, dst, sems, dev):
        return pltpu.make_async_remote_copy(
            src_ref=src, dst_ref=dst, send_sem=sems[0], recv_sem=sems[1],
            device_id=dev, device_id_type=MESH)

    def sp(s, *idx):
        return (s.at[(0,) + idx], s.at[(1,) + idx])

    def cp_q(l):
        return (pltpu.make_async_copy(wq.at[l], wq_b, sem_wq),
                pltpu.make_async_copy(wkv.at[l], wkv_b, sem_wkv))

    def cp_gu(i):
        l, j, s = i // NCH, lax.rem(i, NCH), lax.rem(i, NG)
        cols = pl.ds(pl.multiple_of(j * CH, CH), CH)
        return (pltpu.make_async_copy(wg.at[l, :, cols], wg_b.at[s], sem_g.at[s]),
                pltpu.make_async_copy(wu.at[l, :, cols], wu_b.at[s], sem_u.at[s]))

    def cp_d(i):
        l, j, s = i // NCH, lax.rem(i, NCH), lax.rem(i, ND)
        rows = pl.ds(pl.multiple_of(j * CH, CH), CH)
        return (pltpu.make_async_copy(wd.at[l, rows, :], wd_b.at[s], sem_d.at[s]),)

    def cp_o(l):
        return (pltpu.make_async_copy(wo.at[l], wo_b, sem_wo),)

    def cp_kv(l):
        return (pltpu.make_async_copy(kc.at[l], k_b, sem_k),
                pltpu.make_async_copy(vc.at[l], v_b, sem_v))

    def start(cs):
        for cpy in cs:
            cpy.start()

    def wait(cs):
        for cpy in cs:
            cpy.wait()

    start(cp_q(0))
    for k in range(4):
        start(cp_gu(k))

    rows = hid.shape[0]
    eye = (lax.broadcasted_iota(jnp.int32, (rows, 128), 0)
           == lax.broadcasted_iota(jnp.int32, (rows, 128), 1))

    def row_sums(h):
        ss = jnp.sum(h * h, axis=1, keepdims=True)
        row = jnp.sum(jnp.where(eye, ss, 0.0), axis=0, keepdims=True)
        return jnp.broadcast_to(row, tot.shape)

    me = x * 2 + y
    ss0[me] = row_sums(hid[...].astype(F32))

    def other(k):
        return {"x": lax.rem(x + k // 2, 4), "yz": lax.rem(y + k % 2, 2)}

    with jax.named_scope("barrier"):
        barrier = pltpu.get_barrier_semaphore()
        for k in range(1, 8):
            pl.semaphore_signal(barrier, inc=1, device_id=other(k), device_id_type=MESH)
        pl.semaphore_wait(barrier, 7)

    with jax.named_scope("hx"):
        h_send = rc(hid, hin.at[y], sp(sem_h), dev_y)
        h_send.start()
        s0 = [rc(ss0.at[me], ss0.at[me], sp(sem_s0, k), other(k)) for k in range(1, 8)]
        for cpy in s0:
            cpy.start()
        for k in range(4, NG):
            start(cp_gu(k))
        start(cp_kv(0))
        hin[y] = hid[...]
        rc(hid, hin.at[1 - y], sp(sem_h), dev_y).wait_recv()
        half = hid.shape[1]
        for g in range(2):
            for n in range(2):
                h_b[g, :, n * half:(n + 1) * half] = hin[n, g * (rows // 2):(g + 1) * (rows // 2)]
        h_send.wait_send()
        for cpy in s0:
            cpy.wait_send()
        for k in range(1, 8):
            frm = lax.rem(x + 4 - k // 2, 4) * 2 + lax.rem(y + 2 - k % 2, 2)
            rc(ss0.at[frm], ss0.at[frm], sp(sem_s0, k), other(k)).wait_recv()
        total = ss0[0]
        for k in range(1, 8):
            total = total + ss0[k]
        tot[...] = total

    def sums(k, dev):
        return rc(ss_s, ss_r.at[k], sp(sem_ss, k), dev)

    def send_sums():
        ss_s[...] = row_sums(h_b[...].reshape(rows, 2 * half).astype(F32))
        for k, dev in enumerate((dev_p, dev_q, dev_d)):
            sums(k, dev).start()

    def get_sums():
        for k, dev in enumerate((dev_p, dev_q, dev_d)):
            sums(k, dev).wait()
        tot[...] = (ss_s[...] + ss_r[0]) + (ss_r[1] + ss_r[2])

    def make_u(l, g):
        gall = gain[...].astype(F32)
        gl = gall[0:1]
        for k in range(1, L):
            gl = jnp.where(l == k, gall[k:k + 1], gl)
        u_b[g] = (h_b[g].astype(F32) * (gl * SHRINK)).astype(BF)

    @jax.named_scope("scale")
    def row_scale(l):
        pl.when(l > 0)(get_sums)
        tot_col = jnp.sum(jnp.where(eye, jnp.broadcast_to(tot[0:1], eye.shape), 0.0), axis=1, keepdims=True)
        sc = jnp.broadcast_to(lax.rsqrt(tot_col / D + NORM_EPS) / SHRINK, eye.shape)
        for r in range(4):
            sc_b[r // 2, r % 2] = sc[16 * r:16 * r + 16]

    def scaled(z, g):
        sc = sc_b[g, c][:, 0:1]
        return jnp.where(sc > 0.0, z * sc, 0.0)

    def put_rows(dst, cols, val):
        v = val.astype(BF)
        for r in range(4):
            dst[r // 2, r % 2, :, cols] = v[16 * r:16 * r + 16]

    pieces = (slice(0, QC // 2), slice(QC // 2, QC + HD))

    def to_p_q(k):
        cols = pieces[k]
        return rc(part_q.at[:, 1 - c, :, cols], rb_q.at[:, :, cols], sp(sem_rb, NCH + k), dev_p)

    def to_q_q(k):
        cols = pieces[k]
        return rc(part_q.at[1 - cx, c, :, cols], ib_q.at[:, cols], sp(sem_ib, NCH + k), dev_q)

    @jax.named_scope("a_q")
    def a_q(l):
        wait(cp_q(l))
        u = u_b[...].reshape(rows, u_b.shape[2])
        for k in range(2):
            for n in range(k * QC // 2, (k + 1) * QC // 2, 512):
                put_rows(part_q, slice(n, n + 512), jnp.dot(u, wq_b[:, n:n + 512], preferred_element_type=F32))
            if k == 1:
                put_rows(part_q, slice(QC, QC + HD), jnp.dot(u, wkv_b[...], preferred_element_type=F32))
            to_p_q(k).start()

        @pl.when(l + 1 < L)
        def _():
            start(cp_q(l + 1))

    @jax.named_scope("b_q")
    def b_q(k):
        cols = pieces[k]
        to_p_q(k).wait()
        s = part_q[1 - cx, c, :, cols].astype(F32) + rb_q[1 - cx, :, cols].astype(F32)
        part_q[1 - cx, c, :, cols] = s.astype(BF)
        to_q_q(k).start()

    @jax.named_scope("c_q")
    def c_q(l):
        for k in range(2):
            to_q_q(k).wait()
        z = scaled((part_q[cx, c].astype(F32) + rb_q[cx].astype(F32)) + ib_q[...].astype(F32), cx)
        zq[0] = z[0:8].astype(BF)
        zq[1] = z[8:16].astype(BF)
        rc(zq.at[1 - y], yq.at[y], sp(sem_zq), dev_y).start()
        yq[y] = zq[y]

    @jax.named_scope("attend")
    def attend(l):
        rc(zq.at[1 - y], yq.at[1 - y], sp(sem_zq), dev_y).wait()
        q0 = yq[0].astype(F32)
        q1 = yq[1].astype(F32)
        k_new = q0[:, QC:]
        v_new = q1[:, QC:]
        knew[l] = k_new.astype(BF)
        vnew[l] = v_new.astype(BF)
        nh = QC // HD
        ns = 8
        heads = [qq[:, h * HD:(h + 1) * HD] for qq in (q0, q1) for h in range(nh)]
        qf = jnp.concatenate(heads, axis=0)
        qb = qf.astype(BF)
        nr = 2 * nh * ns
        pos = lax.broadcasted_iota(jnp.int32, (nr, HD), 1)
        seq = lax.rem(lax.broadcasted_iota(jnp.int32, (nr, HD), 0), ns)
        ln = jnp.zeros((nr, HD), jnp.int32)
        for b in range(ns):
            ln = jnp.where(seq == b, lens[b], ln)
        k_rep = jnp.concatenate([k_new] * (2 * nh), axis=0)
        v_rep = jnp.concatenate([v_new] * (2 * nh), axis=0)
        s_new = jnp.sum(qf * k_rep, axis=1, keepdims=True)
        wait(cp_kv(l))
        s = jnp.zeros((nr, HD), F32)
        for b in range(ns):
            sb = lax.dot_general(qb, k_b[b], (((1,), (1,)), ((), ())), preferred_element_type=F32)
            s = jnp.where(seq == b, sb, s)
        s = jnp.where(pos == ln, s_new, s) * HD ** -0.5
        s = jnp.where(pos <= ln, s, -1e30)
        e = jnp.exp(s - jnp.max(s, axis=1, keepdims=True))
        p = (e / jnp.sum(e, axis=1, keepdims=True)).astype(BF).astype(F32)
        p_new = jnp.sum(jnp.where(pos == ln, p, 0.0), axis=1, keepdims=True)
        p_old = jnp.where(pos == ln, 0.0, p)
        o = p_new * v_rep
        for b in range(ns):
            pb = jnp.where(seq == b, p_old, 0.0).astype(BF)
            o = o + jnp.dot(pb, v_b[b], preferred_element_type=F32)
        for hh in range(2):
            for h in range(nh):
                r0 = (hh * nh + h) * ns
                ob[hh, :, h * HD:(h + 1) * HD] = o[r0:r0 + ns].astype(BF)
        rc(ob.at[1 - y], o_all.at[cx, c, y], sp(sem_oy), dev_y).start()
        o_all[cx, c, y] = ob[y]

        @pl.when(l + 1 < L)
        def _():
            start(cp_kv(l + 1))

    @jax.named_scope("o_send")
    def o_send():
        rc(ob.at[1 - y], o_all.at[cx, c, 1 - y], sp(sem_oy), dev_y).wait()
        rc(o_all.at[cx, c], o_all.at[cx, c], sp(sem_op), dev_p).start()
        rc(o_all.at[cx, c], o_all.at[cx, c], sp(sem_oq), dev_q).start()

    @jax.named_scope("o_fwd")
    def o_fwd():
        rc(o_all.at[1 - cx, c], o_all.at[1 - cx, c], sp(sem_oq), dev_q).wait_recv()
        rc(o_all.at[1 - cx, c], o_all.at[1 - cx, c], sp(sem_of), dev_p).start()

    @jax.named_scope("o_all_rows")
    def o_out(l):
        rc(o_all.at[cx, c], o_all.at[cx, 1 - c], sp(sem_op), dev_p).wait()
        rc(o_all.at[1 - cx, c], o_all.at[1 - cx, 1 - c], sp(sem_of), dev_p).wait()
        rc(o_all.at[cx, c], o_all.at[cx, c], sp(sem_oq), dev_q).wait_send()
        wait(cp_o(l))
        blocks = [o_all[i // 4, (i // 2) % 2, i % 2].astype(F32) for i in range(8)]
        lhs = jnp.concatenate(blocks, axis=0).astype(BF)
        hr = rows // 2
        for n in range(0, acc.shape[2], 512):
            v = jnp.dot(lhs, wo_b[:, n:n + 512], preferred_element_type=F32)
            for g in range(2):
                acc[g, :, n:n + 512] += v[g * hr:(g + 1) * hr]

        @pl.when(l + 1 < L)
        def _():
            start(cp_o(l + 1))

    def own(l):
        return lax.rem(cx + l, 2)

    def gu_products(l, j, u, put):
        s = lax.rem(l * NCH + j, NG)
        for n in range(0, CH, 512):
            put(slice(n, n + 512), jnp.dot(u, wg_b[s, :, n:n + 512], preferred_element_type=F32))
            put(slice(CH + n, CH + n + 512), jnp.dot(u, wu_b[s, :, n:n + 512], preferred_element_type=F32))

    def half_rows(l, j, g):
        def put(cols, val):
            v = val.astype(BF)
            for r in range(2):
                part[j, g, r, :, cols] = v[16 * r:16 * r + 16]
        gu_products(l, j, u_b[g], put)

    def next_gu(i):
        @pl.when(i + NG < L * NCH)
        def _():
            start(cp_gu(i + NG))

    def to_p(j):
        return rc(part.at[j, :, 1 - c], rb.at[j], sp(sem_rb, j), dev_p)

    def to_p_half(j, g, k):
        return rc(part.at[j, g, 1 - c], rb.at[j, g], sp(sem_rb, k), dev_p)

    def to_q(l, j):
        return rc(part.at[j, 1 - own(l), c], ib.at[j], sp(sem_ib, j), dev_q)

    @jax.named_scope("a_early")
    def a_early(l, j):
        wait(cp_gu(l * NCH + j))
        half_rows(l, j, 1 - own(l))
        to_p_half(j, 1 - own(l), j).start()

    @jax.named_scope("a_late")
    def a_late(l, j):
        half_rows(l, j, own(l))
        to_p_half(j, own(l), NCH + 2 + j).start()
        next_gu(l * NCH + j)

    @jax.named_scope("stage_a")
    def stage_a(l, j):
        i = l * NCH + j
        wait(cp_gu(i))
        dst = part.at[j]
        gu_products(l, j, u_b[...].reshape(rows, u_b.shape[2]), lambda cols, val: put_rows(dst, cols, val))
        to_p(j).start()
        next_gu(i)

    def add_to_q(l, j):
        g = 1 - own(l)
        s = part[j, g, c].astype(F32) + rb[j, g].astype(F32)
        part[j, g, c] = s.astype(BF)
        to_q(l, j).start()

    @jax.named_scope("b_early")
    def b_early(l, j):
        to_p_half(j, 1 - own(l), j).wait()
        add_to_q(l, j)

    @jax.named_scope("stage_b")
    def stage_b(l, j):
        to_p(j).wait()
        add_to_q(l, j)

    @jax.named_scope("stage_c")
    def stage_c(l, j):
        g = own(l)

        @pl.when(j < NE)
        def _():
            to_p_half(j, g, NCH + 2 + j).wait()

        to_q(l, j).wait()
        z = (part[j, g, c].astype(F32) + rb[j, g].astype(F32)) + ib[j].astype(F32)
        z = scaled(z, g).astype(BF).astype(F32)
        gate, up = z[:, :CH], z[:, CH:]
        m_all[j, g, c] = (jax.nn.silu(gate) * up).astype(BF)
        m_send(j, g, sem_mq, dev_q).start()

        @pl.when(j == NCH - 1)
        def _():
            m_send(j, g, sem_mf, dev_d).start()

        m_send(j, g, sem_mp, dev_p).start()

    def m_send(j, g, sem, dev):
        return rc(m_all.at[j, g, c], m_all.at[j, g, c], sp(sem, j), dev)

    def m_from(j, g, cc, sem, dev):
        return rc(m_all.at[j, g, cc], m_all.at[j, g, cc], sp(sem, j), dev)

    @jax.named_scope("stage_d")
    def stage_d(l, j):
        g = 1 - own(l)
        m_from(j, g, c, sem_mq, dev_q).wait_recv()
        m_send(j, g, sem_mf, dev_p).start()

    def e_rows(s, j, g):
        m = m_all[j, g].reshape(rows // 2, CH)
        for n in range(0, acc.shape[2], 512):
            acc[g, :, n:n + 512] += jnp.dot(m, wd_b[s, :, n:n + 512], preferred_element_type=F32)

    def near_in(l, j):
        m_send(j, own(l), sem_mp, dev_p).wait_send()
        m_from(j, own(l), 1 - c, sem_mp, dev_p).wait_recv()
        wait(cp_d(l * NCH + j))

    def far_in(l, j):
        g = 1 - own(l)
        m_send(j, g, sem_mf, dev_p).wait_send()
        m_from(j, g, 1 - c, sem_mf, dev_p).wait_recv()
        m_send(j, own(l), sem_mq, dev_q).wait_send()

    def next_d(i):
        @pl.when(i + ND < L * NCH)
        def _():
            start(cp_d(i + ND))

    @jax.named_scope("e_all")
    def e_all(l, j):
        i = l * NCH + j
        near_in(l, j)
        far_in(l, j)
        s = lax.rem(i, ND)
        m = m_all[j].reshape(rows, CH)
        hr = rows // 2
        for n in range(0, acc.shape[2], 512):
            v = jnp.dot(m, wd_b[s, :, n:n + 512], preferred_element_type=F32)
            for g in range(2):
                acc[g, :, n:n + 512] += v[g * hr:(g + 1) * hr]
        next_d(i)

    @jax.named_scope("e_near")
    def e_near(l, j):
        near_in(l, j)
        e_rows(lax.rem(l * NCH + j, ND), j, own(l))

    @jax.named_scope("e_far")
    def e_far(l, j):
        i = l * NCH + j
        far_in(l, j)
        e_rows(lax.rem(i, ND), j, 1 - own(l))
        next_d(i)

    @jax.named_scope("take_rows")
    def take_rows(g):
        for n in range(2):
            yx(g, n).wait_recv()
        for n in range(2):
            cols = slice(n * half, (n + 1) * half)
            upd = yx_s[g, n].astype(F32) + yx_r[g, n].astype(F32)
            h_b[g, :, cols] = (h_b[g, :, cols].astype(F32) + upd).astype(BF)

    @jax.named_scope("last_sends")
    def last_sends(l):
        j = NCH - 1
        m_send(j, own(l), sem_mq, dev_q).wait_send()
        m_send(j, own(l), sem_mf, dev_d).wait_send()
        for g in range(2):
            yx(g, 1 - y).wait_send()
            pl.when(l + 1 < L)(lambda: yx(g, y).wait_send())

    def layer(l, carry):
        early = 1 - own(l)

        @pl.when(l > 0)
        def _():
            take_rows(early)

        make_u(l, early)
        a_early(l, 0)
        a_early(l, 1)
        b_early(l, 0)
        a_early(l, 2)
        b_early(l, 1)

        @pl.when(l > 0)
        def _():
            take_rows(1 - early)
            send_sums()

        make_u(l, 1 - early)
        a_q(l)
        acc[...] = jnp.zeros_like(acc)
        pl.when(l > 0)(lambda: last_sends(l - 1))

        def step(t, carry2):
            def at(steps, fn, first=0):
                if isinstance(steps, int):
                    pl.when(t == steps)(fn)
                    return
                hit = t == steps[0]
                j = jnp.int32(first)
                for k, st in enumerate(steps[1:]):
                    hit = hit | (t == st)
                    j = jnp.where(t >= st, first + k + 1, j)
                pl.when(hit)(lambda: fn(j))

            at(T_A, lambda j: stage_a(l, j), NE)
            at(T_AL, lambda j: a_late(l, j))
            pl.when((l == 0) & (t < ND))(lambda: start(cp_d(t)))
            pl.when((l == 0) & (t == 3))(lambda: start(cp_o(0)))
            at(T_QB, lambda: b_q(0))
            at(T_QB, lambda: b_q(1))
            at(T_QB, lambda: b_early(l, 2))
            at(T_B, lambda j: stage_b(l, j), NE)
            at(T_SC, lambda: row_scale(l))
            at(T_QC, lambda: c_q(l))
            at(T_D, lambda j: stage_d(l, j))
            at(T_OE, lambda: o_out(l))
            at(T_LN, lambda: last_near(l))
            at(T_EA, lambda j: e_all(l, j))
            at(T_OS, o_send)
            at(T_C1, lambda j: stage_c(l, j), C1)
            at(T_C2, lambda j: stage_c(l, j), C2)
            at(T_C3, lambda j: stage_c(l, j), C3)
            at(T_EN, lambda j: e_near(l, j), NF)
            at(T_EF, lambda j: e_far(l, j), NF)
            at(T_OF, o_fwd)
            at(T_ATT, lambda: attend(l))
            return carry2

        lax.fori_loop(0, STEPS, step, 0)
        last_far(l)
        return carry

    def yx(g, n):
        return rc(yx_s.at[g, n], yx_r.at[g, n], sp(sem_yx, g, n), dev_y)

    def last_rows(l, s, g):
        m = m_all[NCH - 1, g].reshape(rows // 2, CH)
        for n in (1 - y, y):
            cols = pl.ds(pl.multiple_of(n * half, half), half)
            v = acc[g, :, cols] + jnp.dot(m, wd_b[s, :, cols], preferred_element_type=F32)
            yx_s[g, n] = v.astype(BF)
            if n is y:
                pl.when(l + 1 < L)(lambda: yx(g, y).start())
            else:
                yx(g, n).start()

    @jax.named_scope("last_near")
    def last_near(l):
        j = NCH - 1
        near_in(l, j)
        last_rows(l, lax.rem(l * NCH + j, ND), own(l))

    @jax.named_scope("last_far")
    def last_far(l):
        j = NCH - 1
        i = l * NCH + j
        g = 1 - own(l)
        m_from(j, g, c, sem_mq, dev_q).wait_recv()
        m_from(j, g, 1 - c, sem_mf, dev_d).wait_recv()
        last_rows(l, lax.rem(i, ND), g)
        next_d(i)

    @jax.named_scope("swap")
    def finish():
        hr = rows // 2
        for g in range(2):
            yx(g, y).wait_recv()
            cols = pl.ds(pl.multiple_of(y * half, half), half)
            upd = yx_s[g, y].astype(F32) + yx_r[g, y].astype(F32)
            hout[g * hr:(g + 1) * hr, :] = (h_b[g, :, cols].astype(F32) + upd).astype(BF)
        last_sends(jnp.int32(L - 1))

    lax.fori_loop(0, L, layer, 0)
    finish()


def place_kernel(kn, vn, hn, kc, vc, lens, ko, vo, ho, new_b, h_b, kv_b, sem_n, sem_h, sem_in, sem_out):
    L, ns, _, hd = kc.shape
    T = 16
    pairs = [(a, l) for l in range(L) for a in range(2)]
    news = [pltpu.make_async_copy((kn, vn)[a], new_b.at[a], sem_n.at[a]) for a in range(2)]
    h_in = pltpu.make_async_copy(hn, h_b, sem_h)
    ins = [pltpu.make_async_copy((kc, vc)[a].at[l], kv_b.at[a, l], sem_in.at[a, l]) for a, l in pairs]
    outs = [pltpu.make_async_copy(kv_b.at[a, l], (ko, vo)[a].at[l], sem_out.at[a, l]) for a, l in pairs]
    for cpy in news + ins + [h_in]:
        cpy.start()
    for cpy in news:
        cpy.wait()
    row = lax.broadcasted_iota(jnp.int32, (T, hd), 0)
    for k, (a, l) in enumerate(pairs):
        ins[k].wait()
        for b in range(ns):
            base = pl.multiple_of(lens[b] // T * T, T)
            tile = kv_b[a, l, b, pl.ds(base, T), :].astype(F32)
            new = new_b[a, l, b:b + 1, :].astype(F32)
            kv_b[a, l, b, pl.ds(base, T), :] = jnp.where(row == lens[b] - base, new, tile).astype(BF)
        outs[k].start()
    h_in.wait()
    h_out = pltpu.make_async_copy(h_b, ho, sem_h)
    h_out.start()
    for cpy in outs + [h_out]:
        cpy.wait()


def solution(mesh):
    row_spec = P("dp", ("x", "yz"))
    tile_in = P(None, "x", "yz")
    tile_out = P(None, "yz", "x")
    cache_spec = P(None, ("dp", "x", "yz"))
    len_spec = P(("dp", "x", "yz"))

    def device_step(hidden, norm_gain, w_q, w_kv, w_gate, w_up, w_o, w_down, k_cache, v_cache, seq_len):
        L, k_in, q_cols = w_q.shape
        rows = hidden.shape[0]
        half = hidden.shape[1]
        kv_cols = w_kv.shape[2]
        ff = w_gate.shape[2]
        ch = CH
        nch = ff // ch
        d_out = w_o.shape[2]
        ns, cache_len, hd = k_cache.shape[1:]
        zc = q_cols + kv_cols
        dims = {"layers": L, "n_chunks": nch, "d": half * 8}
        vm = pl.BlockSpec(memory_space=pltpu.VMEM)
        anyspec = pl.BlockSpec(memory_space=pl.ANY)
        DMA = pltpu.SemaphoreType.DMA
        V = pltpu.VMEM
        h_new, k_new, v_new = pl.pallas_call(
            functools.partial(step_kernel, dims),
            out_shape=(
                jax.ShapeDtypeStruct(hidden.shape, BF),
                jax.ShapeDtypeStruct((L, ns, hd), BF),
                jax.ShapeDtypeStruct((L, ns, hd), BF),
            ),
            in_specs=[vm, vm] + [anyspec] * 8 + [pl.BlockSpec(memory_space=pltpu.SMEM)],
            out_specs=(vm, vm, vm),
            scratch_shapes=[
                V((k_in, q_cols), BF), V((k_in, kv_cols), BF),
                V((NG, k_in, ch), BF), V((NG, k_in, ch), BF),
                V((q_cols, d_out), BF), V((ND, ch, d_out), BF),
                V((ns, cache_len, hd), BF), V((ns, cache_len, hd), BF),
                V((2, rows, half), BF), V((2, rows // 2, d_out), BF), V((2, rows // 2, d_out), BF), V((2, rows // 2, d_out), F32),
                V((8, 128), F32), V((3, 8, 128), F32), V((8, 8, 128), F32), V((8, 128), F32), V((2, 2, 16, 128), F32),
                V((nch, 2, 2, 16, 2 * ch), BF), V((nch, 2, 16, 2 * ch), BF), V((nch, 16, 2 * ch), BF),
                V((nch, 2, 2, 16, ch), BF),
                V((2, 2, 16, zc), BF), V((2, 16, zc), BF), V((16, zc), BF),
                V((2, ns, zc), BF), V((2, ns, zc), BF),
                V((2, ns, q_cols), BF), V((2, 2, 2, ns, q_cols), BF),
                V((2, 2, rows // 2, half), BF), V((2, 2, rows // 2, half), BF),
                DMA, DMA, DMA((NG,)), DMA((NG,)), DMA, DMA((ND,)), DMA, DMA,
                DMA((2,)), DMA((2, 8)), DMA((2, 3)), DMA((2, nch + 2 + NE)), DMA((2, nch + 2)),
                DMA((2, nch)), DMA((2, nch)), DMA((2, nch)),
                DMA((2,)), DMA((2,)), DMA((2,)), DMA((2,)), DMA((2,)), DMA((2, 2, 2)),
            ],
            compiler_params=pltpu.CompilerParams(
                collective_id=0, has_side_effects=True, vmem_limit_bytes=67_000_000),
            name="decode_step",
        )(hidden, norm_gain, w_q, w_kv, w_gate, w_up, w_o, w_down, k_cache, v_cache, seq_len)
        k_out, v_out, h_out = pl.pallas_call(
            place_kernel,
            out_shape=(
                jax.ShapeDtypeStruct(k_cache.shape, BF),
                jax.ShapeDtypeStruct(v_cache.shape, BF),
                jax.ShapeDtypeStruct(hidden.shape, BF),
            ),
            in_specs=[anyspec] * 5 + [pl.BlockSpec(memory_space=pltpu.SMEM)],
            out_specs=(anyspec,) * 3,
            scratch_shapes=[
                V((2, L, ns, hd), BF), V((rows, half), BF), V((2, L, ns, cache_len, hd), BF),
                DMA((2,)), DMA, DMA((2, L)), DMA((2, L)),
            ],
            compiler_params=pltpu.CompilerParams(vmem_limit_bytes=60_000_000),
            name="place_rows",
        )(k_new, v_new, h_new, k_cache, v_cache, seq_len)
        return h_out, k_out, v_out

    return jax.shard_map(
        device_step,
        mesh=mesh,
        in_specs=(row_spec, P(None, "x"), tile_in, tile_in, tile_in, tile_in, tile_out, tile_out, cache_spec, cache_spec, len_spec),
        out_specs=(row_spec, cache_spec, cache_spec),
        check_vma=False,
    )
```

```python
import functools

import jax
import jax.numpy as jnp
from jax import lax
from jax.experimental import pallas as pl
from jax.experimental.pallas import tpu as pltpu
from jax.sharding import PartitionSpec as P

NORM_EPS = 1e-6
SHRINK = 2.0 ** -64
MESH = pl.DeviceIdType.MESH
BF = jnp.bfloat16
F32 = jnp.float32

CH = 1024
NG = 7
ND = 8
NE = 3
NF = 4
T_A = (0, 1, 5, 6, 7)
T_AL = (2, 3, 4)
T_B = (1, 2, 6, 7, 8)
C1, C2, C3 = 0, 5, 6
T_C1, T_C2, T_C3 = (4, 5, 6, 7, 8), (10,), (11, 13)
T_D = (9, 10, 11, 13, 14, 15)
T_EA = (10, 11, 12, 14)
T_EN = (10, 12, 13)
T_EF = (15, 16, 17)
T_SC, T_QB, T_QC, T_ATT, T_OS, T_OF, T_OE, T_LN = 4, 0, 4, 7, 10, 14, 15, 15
T_ON, T_LN0 = 13, 14
STEPS = 18


def step_kernel(dims, hid, gain, wq, wkv, wg, wu, wo, wd, kc, vc, lens,
                hout, knew, vnew,
                wq_b, wkv_b, wg_b, wu_b, wo_b, wd_b, k_b, v_b,
                hin, h_b, u_b, acc, ss_s, ss_r, tot, sc_b,
                part, rb, ib, m_all, part_q, rb_q, ib_q, zq, yq, ob, o_all, yx_s, yx_r,
                sem_wq, sem_wkv, sem_g, sem_u, sem_wo, sem_d, sem_k, sem_v,
                sem_h, sem_ss, sem_rb, sem_ib, sem_mp, sem_mq, sem_mf,
                sem_zq, sem_oy, sem_op, sem_oq, sem_of, sem_yx):
    L, NCH, D = dims["layers"], dims["n_chunks"], dims["d"]
    HD = 256
    QC = wq_b.shape[1]
    x = lax.axis_index("x")
    y = lax.axis_index("yz")
    c = lax.rem(x, 2)
    cx = x // 2
    xp = x + 1 - 2 * c
    xq = lax.rem(x + 2, 4)
    xd = 3 - x
    dev_p, dev_q, dev_d, dev_y = {"x": xp}, {"x": xq}, {"x": xd}, {"yz": 1 - y}

    def rc(src, dst, sems, dev):
        return pltpu.make_async_remote_copy(
            src_ref=src, dst_ref=dst, send_sem=sems[0], recv_sem=sems[1],
            device_id=dev, device_id_type=MESH)

    def sp(s, *idx):
        return (s.at[(0,) + idx], s.at[(1,) + idx])

    def cp_q(l):
        return (pltpu.make_async_copy(wq.at[l], wq_b, sem_wq),
                pltpu.make_async_copy(wkv.at[l], wkv_b, sem_wkv))

    def cp_gu(i):
        l, j, s = i // NCH, lax.rem(i, NCH), lax.rem(i, NG)
        cols = pl.ds(pl.multiple_of(j * CH, CH), CH)
        return (pltpu.make_async_copy(wg.at[l, :, cols], wg_b.at[s], sem_g.at[s]),
                pltpu.make_async_copy(wu.at[l, :, cols], wu_b.at[s], sem_u.at[s]))

    def cp_d(i):
        l, j, s = i // NCH, lax.rem(i, NCH), lax.rem(i, ND)
        rows = pl.ds(pl.multiple_of(j * CH, CH), CH)
        return (pltpu.make_async_copy(wd.at[l, rows, :], wd_b.at[s], sem_d.at[s]),)

    def cp_o(l):
        return (pltpu.make_async_copy(wo.at[l], wo_b, sem_wo),)

    def cp_kv(l):
        return (pltpu.make_async_copy(kc.at[l], k_b, sem_k),
                pltpu.make_async_copy(vc.at[l], v_b, sem_v))

    def start(cs):
        for cpy in cs:
            cpy.start()

    def wait(cs):
        for cpy in cs:
            cpy.wait()

    start(cp_q(0))
    for k in range(4):
        start(cp_gu(k))

    rows = hid.shape[0]
    eye = (lax.broadcasted_iota(jnp.int32, (rows, 128), 0)
           == lax.broadcasted_iota(jnp.int32, (rows, 128), 1))

    def row_sums(h):
        ss = jnp.sum(h * h, axis=1, keepdims=True)
        row = jnp.sum(jnp.where(eye, ss, 0.0), axis=0, keepdims=True)
        return jnp.broadcast_to(row, tot.shape)

    with jax.named_scope("barrier"):
        barrier = pltpu.get_barrier_semaphore()
        for dev in (dev_p, dev_q, dev_d, dev_y):
            pl.semaphore_signal(barrier, inc=1, device_id=dev, device_id_type=MESH)
        pl.semaphore_wait(barrier, 4)

    with jax.named_scope("hx"):
        half = hid.shape[1]
        hr = rows // 2

        def h_rows(g, yy):
            return rc(hid.at[pl.ds(pl.multiple_of(g * hr, hr), hr)], hin.at[yy, g], sp(sem_h, g), dev_y)

        h_rows(1 - cx, y).start()
        h_rows(cx, y).start()
        for k in range(4, NG):
            start(cp_gu(k))
        start(cp_kv(0))
        for g in range(2):
            hin[y, g] = hid[g * hr:(g + 1) * hr]

    @jax.named_scope("first_rows")
    def first_rows(g):
        h_rows(g, 1 - y).wait_recv()
        for n in range(2):
            h_b[g, :, n * half:(n + 1) * half] = hin[n, g]

    def sums(k, dev):
        return rc(ss_s, ss_r.at[k], sp(sem_ss, k), dev)

    def send_sums():
        ss_s[...] = row_sums(h_b[...].reshape(rows, 2 * half).astype(F32))
        for k, dev in enumerate((dev_p, dev_q, dev_d)):
            sums(k, dev).start()

    def get_sums():
        for k, dev in enumerate((dev_p, dev_q, dev_d)):
            sums(k, dev).wait()
        tot[...] = (ss_s[...] + ss_r[0]) + (ss_r[1] + ss_r[2])

    def make_u(l, g):
        gall = gain[...].astype(F32)
        gl = gall[0:1]
        for k in range(1, L):
            gl = jnp.where(l == k, gall[k:k + 1], gl)
        u_b[g] = (h_b[g].astype(F32) * (gl * SHRINK)).astype(BF)

    @jax.named_scope("scale")
    def row_scale(l):
        get_sums()
        tot_col = jnp.sum(jnp.where(eye, jnp.broadcast_to(tot[0:1], eye.shape), 0.0), axis=1, keepdims=True)
        sc = jnp.broadcast_to(lax.rsqrt(tot_col / D + NORM_EPS) / SHRINK, eye.shape)
        for r in range(4):
            sc_b[r // 2, r % 2] = sc[16 * r:16 * r + 16]

    def scaled(z, g):
        sc = sc_b[g, c][:, 0:1]
        return jnp.where(sc > 0.0, z * sc, 0.0)

    def put_rows(dst, cols, val):
        v = val.astype(BF)
        for r in range(4):
            dst[r // 2, r % 2, :, cols] = v[16 * r:16 * r + 16]

    pieces = (slice(0, QC // 2), slice(QC // 2, QC + HD))

    def to_p_q(k):
        cols = pieces[k]
        return rc(part_q.at[:, 1 - c, :, cols], rb_q.at[:, :, cols], sp(sem_rb, NCH + k), dev_p)

    def to_q_q(k):
        cols = pieces[k]
        return rc(part_q.at[1 - cx, c, :, cols], ib_q.at[:, cols], sp(sem_ib, NCH + k), dev_q)

    @jax.named_scope("a_q")
    def a_q(l):
        wait(cp_q(l))
        u = u_b[...].reshape(rows, u_b.shape[2])
        for k in range(2):
            for n in range(k * QC // 2, (k + 1) * QC // 2, 512):
                put_rows(part_q, slice(n, n + 512), jnp.dot(u, wq_b[:, n:n + 512], preferred_element_type=F32))
            if k == 1:
                put_rows(part_q, slice(QC, QC + HD), jnp.dot(u, wkv_b[...], preferred_element_type=F32))
            to_p_q(k).start()

        @pl.when(l + 1 < L)
        def _():
            start(cp_q(l + 1))

    @jax.named_scope("b_q")
    def b_q(k):
        cols = pieces[k]
        to_p_q(k).wait()
        s = part_q[1 - cx, c, :, cols].astype(F32) + rb_q[1 - cx, :, cols].astype(F32)
        part_q[1 - cx, c, :, cols] = s.astype(BF)
        to_q_q(k).start()

    @jax.named_scope("c_q")
    def c_q(l):
        for k in range(2):
            to_q_q(k).wait()
        z = scaled((part_q[cx, c].astype(F32) + rb_q[cx].astype(F32)) + ib_q[...].astype(F32), cx)
        zq[0] = z[0:8].astype(BF)
        zq[1] = z[8:16].astype(BF)
        rc(zq.at[1 - y], yq.at[y], sp(sem_zq), dev_y).start()
        yq[y] = zq[y]

    @jax.named_scope("attend")
    def attend(l):
        rc(zq.at[1 - y], yq.at[1 - y], sp(sem_zq), dev_y).wait()
        q0 = yq[0].astype(F32)
        q1 = yq[1].astype(F32)
        k_new = q0[:, QC:]
        v_new = q1[:, QC:]
        knew[l] = k_new.astype(BF)
        vnew[l] = v_new.astype(BF)
        nh = QC // HD
        ns = 8
        heads = [qq[:, h * HD:(h + 1) * HD] for qq in (q0, q1) for h in range(nh)]
        qf = jnp.concatenate(heads, axis=0)
        qb = qf.astype(BF)
        nr = 2 * nh * ns
        pos = lax.broadcasted_iota(jnp.int32, (nr, HD), 1)
        seq = lax.rem(lax.broadcasted_iota(jnp.int32, (nr, HD), 0), ns)
        ln = jnp.zeros((nr, HD), jnp.int32)
        for b in range(ns):
            ln = jnp.where(seq == b, lens[b], ln)
        k_rep = jnp.concatenate([k_new] * (2 * nh), axis=0)
        v_rep = jnp.concatenate([v_new] * (2 * nh), axis=0)
        s_new = jnp.sum(qf * k_rep, axis=1, keepdims=True)
        wait(cp_kv(l))
        s = jnp.zeros((nr, HD), F32)
        for b in range(ns):
            sb = lax.dot_general(qb, k_b[b], (((1,), (1,)), ((), ())), preferred_element_type=F32)
            s = jnp.where(seq == b, sb, s)
        s = jnp.where(pos == ln, s_new, s) * HD ** -0.5
        s = jnp.where(pos <= ln, s, -1e30)
        e = jnp.exp(s - jnp.max(s, axis=1, keepdims=True))
        p = (e / jnp.sum(e, axis=1, keepdims=True)).astype(BF).astype(F32)
        p_new = jnp.sum(jnp.where(pos == ln, p, 0.0), axis=1, keepdims=True)
        p_old = jnp.where(pos == ln, 0.0, p)
        o = p_new * v_rep
        for b in range(ns):
            pb = jnp.where(seq == b, p_old, 0.0).astype(BF)
            o = o + jnp.dot(pb, v_b[b], preferred_element_type=F32)
        for hh in range(2):
            for h in range(nh):
                r0 = (hh * nh + h) * ns
                ob[hh, :, h * HD:(h + 1) * HD] = o[r0:r0 + ns].astype(BF)
        rc(ob.at[1 - y], o_all.at[cx, c, y], sp(sem_oy), dev_y).start()
        o_all[cx, c, y] = ob[y]

        @pl.when(l + 1 < L)
        def _():
            start(cp_kv(l + 1))

    @jax.named_scope("o_send")
    def o_send():
        rc(ob.at[1 - y], o_all.at[cx, c, 1 - y], sp(sem_oy), dev_y).wait()
        rc(o_all.at[cx, c], o_all.at[cx, c], sp(sem_op), dev_p).start()
        rc(o_all.at[cx, c], o_all.at[cx, c], sp(sem_oq), dev_q).start()

    @jax.named_scope("o_fwd")
    def o_fwd():
        rc(o_all.at[1 - cx, c], o_all.at[1 - cx, c], sp(sem_oq), dev_q).wait_recv()
        rc(o_all.at[1 - cx, c], o_all.at[1 - cx, c], sp(sem_of), dev_p).start()

    def o_near_in(l):
        rc(o_all.at[cx, c], o_all.at[cx, 1 - c], sp(sem_op), dev_p).wait()
        wait(cp_o(l))

    def o_far_in():
        rc(o_all.at[1 - cx, c], o_all.at[1 - cx, 1 - c], sp(sem_of), dev_p).wait()
        rc(o_all.at[cx, c], o_all.at[cx, c], sp(sem_oq), dev_q).wait_send()

    def next_o(l):
        @pl.when(l + 1 < L)
        def _():
            start(cp_o(l + 1))

    def o_rows(g):
        lhs = jnp.concatenate([o_all[g, i // 2, i % 2].astype(F32) for i in range(4)], axis=0).astype(BF)
        for n in range(0, acc.shape[2], 512):
            acc[g, :, n:n + 512] += jnp.dot(lhs, wo_b[:, n:n + 512], preferred_element_type=F32)

    @jax.named_scope("o_near")
    def o_near(l):
        o_near_in(l)
        o_rows(cx)

    @jax.named_scope("o_far")
    def o_far(l):
        o_far_in()
        o_rows(1 - cx)
        next_o(l)

    @jax.named_scope("o_all_rows")
    def o_out(l):
        o_near_in(l)
        o_far_in()
        blocks = [o_all[i // 4, (i // 2) % 2, i % 2].astype(F32) for i in range(8)]
        lhs = jnp.concatenate(blocks, axis=0).astype(BF)
        hr = rows // 2
        for n in range(0, acc.shape[2], 512):
            v = jnp.dot(lhs, wo_b[:, n:n + 512], preferred_element_type=F32)
            for g in range(2):
                acc[g, :, n:n + 512] += v[g * hr:(g + 1) * hr]
        next_o(l)

    def own(l):
        return lax.rem(cx + l, 2)

    def gu_products(l, j, u, put):
        s = lax.rem(l * NCH + j, NG)
        for n in range(0, CH, 512):
            put(slice(n, n + 512), jnp.dot(u, wg_b[s, :, n:n + 512], preferred_element_type=F32))
            put(slice(CH + n, CH + n + 512), jnp.dot(u, wu_b[s, :, n:n + 512], preferred_element_type=F32))

    def half_rows(l, j, g):
        def put(cols, val):
            v = val.astype(BF)
            for r in range(2):
                part[j, g, r, :, cols] = v[16 * r:16 * r + 16]
        gu_products(l, j, u_b[g], put)

    def next_gu(i):
        @pl.when(i + NG < L * NCH)
        def _():
            start(cp_gu(i + NG))

    def to_p(j):
        return rc(part.at[j, :, 1 - c], rb.at[j], sp(sem_rb, j), dev_p)

    def to_p_half(j, g, k):
        return rc(part.at[j, g, 1 - c], rb.at[j, g], sp(sem_rb, k), dev_p)

    def to_q(l, j):
        return rc(part.at[j, 1 - own(l), c], ib.at[j], sp(sem_ib, j), dev_q)

    @jax.named_scope("a_early")
    def a_early(l, j):
        wait(cp_gu(l * NCH + j))
        half_rows(l, j, 1 - own(l))
        to_p_half(j, 1 - own(l), j).start()

    @jax.named_scope("a_late")
    def a_late(l, j):
        half_rows(l, j, own(l))
        to_p_half(j, own(l), NCH + 2 + j).start()
        next_gu(l * NCH + j)

    @jax.named_scope("stage_a")
    def stage_a(l, j):
        i = l * NCH + j
        wait(cp_gu(i))
        dst = part.at[j]
        gu_products(l, j, u_b[...].reshape(rows, u_b.shape[2]), lambda cols, val: put_rows(dst, cols, val))
        to_p(j).start()
        next_gu(i)

    def add_to_q(l, j):
        g = 1 - own(l)
        s = part[j, g, c].astype(F32) + rb[j, g].astype(F32)
        part[j, g, c] = s.astype(BF)
        to_q(l, j).start()

    @jax.named_scope("b_early")
    def b_early(l, j):
        to_p_half(j, 1 - own(l), j).wait()
        add_to_q(l, j)

    @jax.named_scope("stage_b")
    def stage_b(l, j):
        to_p(j).wait()
        add_to_q(l, j)

    @jax.named_scope("stage_c")
    def stage_c(l, j):
        g = own(l)

        @pl.when(j < NE)
        def _():
            to_p_half(j, g, NCH + 2 + j).wait()

        to_q(l, j).wait()
        z = (part[j, g, c].astype(F32) + rb[j, g].astype(F32)) + ib[j].astype(F32)
        z = scaled(z, g).astype(BF).astype(F32)
        gate, up = z[:, :CH], z[:, CH:]
        m_all[j, g, c] = (jax.nn.silu(gate) * up).astype(BF)
        m_send(j, g, sem_mq, dev_q).start()

        @pl.when(j == NCH - 1)
        def _():
            m_send(j, g, sem_mf, dev_d).start()

        m_send(j, g, sem_mp, dev_p).start()

    def m_send(j, g, sem, dev):
        return rc(m_all.at[j, g, c], m_all.at[j, g, c], sp(sem, j), dev)

    def m_from(j, g, cc, sem, dev):
        return rc(m_all.at[j, g, cc], m_all.at[j, g, cc], sp(sem, j), dev)

    @jax.named_scope("stage_d")
    def stage_d(l, j):
        g = 1 - own(l)
        m_from(j, g, c, sem_mq, dev_q).wait_recv()
        m_send(j, g, sem_mf, dev_p).start()

    def e_rows(s, j, g):
        m = m_all[j, g].reshape(rows // 2, CH)
        for n in range(0, acc.shape[2], 512):
            acc[g, :, n:n + 512] += jnp.dot(m, wd_b[s, :, n:n + 512], preferred_element_type=F32)

    def near_in(l, j):
        m_send(j, own(l), sem_mp, dev_p).wait_send()
        m_from(j, own(l), 1 - c, sem_mp, dev_p).wait_recv()
        wait(cp_d(l * NCH + j))

    def far_in(l, j):
        g = 1 - own(l)
        m_send(j, g, sem_mf, dev_p).wait_send()
        m_from(j, g, 1 - c, sem_mf, dev_p).wait_recv()
        m_send(j, own(l), sem_mq, dev_q).wait_send()

    def next_d(i):
        @pl.when(i + ND < L * NCH)
        def _():
            start(cp_d(i + ND))

    @jax.named_scope("e_all")
    def e_all(l, j):
        i = l * NCH + j
        near_in(l, j)
        far_in(l, j)
        s = lax.rem(i, ND)
        m = m_all[j].reshape(rows, CH)
        hr = rows // 2
        for n in range(0, acc.shape[2], 512):
            v = jnp.dot(m, wd_b[s, :, n:n + 512], preferred_element_type=F32)
            for g in range(2):
                acc[g, :, n:n + 512] += v[g * hr:(g + 1) * hr]
        next_d(i)

    @jax.named_scope("e_near")
    def e_near(l, j):
        near_in(l, j)
        e_rows(lax.rem(l * NCH + j, ND), j, own(l))

    @jax.named_scope("e_far")
    def e_far(l, j):
        i = l * NCH + j
        far_in(l, j)
        e_rows(lax.rem(i, ND), j, 1 - own(l))
        next_d(i)

    @jax.named_scope("take_rows")
    def take_rows(g):
        for n in range(2):
            yx(g, n).wait_recv()
        for n in range(2):
            cols = slice(n * half, (n + 1) * half)
            upd = yx_s[g, n].astype(F32) + yx_r[g, n].astype(F32)
            h_b[g, :, cols] = (h_b[g, :, cols].astype(F32) + upd).astype(BF)

    @jax.named_scope("last_sends")
    def last_sends(l):
        j = NCH - 1
        m_send(j, own(l), sem_mq, dev_q).wait_send()
        m_send(j, own(l), sem_mf, dev_d).wait_send()
        for g in range(2):
            yx(g, 1 - y).wait_send()
            pl.when(l + 1 < L)(lambda: yx(g, y).wait_send())

    def layer(l, carry):
        early = 1 - own(l)

        pl.when(l == 0)(lambda: first_rows(early))
        pl.when(l > 0)(lambda: take_rows(early))
        make_u(l, early)
        a_early(l, 0)
        a_early(l, 1)
        b_early(l, 0)
        a_early(l, 2)
        b_early(l, 1)

        pl.when(l == 0)(lambda: first_rows(1 - early))
        pl.when(l > 0)(lambda: take_rows(1 - early))
        send_sums()
        make_u(l, 1 - early)
        a_q(l)
        acc[...] = jnp.zeros_like(acc)
        pl.when(l > 0)(lambda: last_sends(l - 1))

        @pl.when(l == 0)
        def _():
            for g in range(2):
                h_rows(g, y).wait_send()

        def step(t, carry2):
            def at(steps, fn, first=0, t=t):
                if isinstance(steps, int):
                    pl.when(t == steps)(fn)
                    return
                hit = t == steps[0]
                j = jnp.int32(first)
                for k, st in enumerate(steps[1:]):
                    hit = hit | (t == st)
                    j = jnp.where(t >= st, first + k + 1, j)
                pl.when(hit)(lambda: fn(j))

            at(T_A, lambda j: stage_a(l, j), NE)
            at(T_AL, lambda j: a_late(l, j))
            pl.when((l == 0) & (t < ND))(lambda: start(cp_d(t)))
            pl.when((l == 0) & (t == 3))(lambda: start(cp_o(0)))
            at(T_QB, lambda: b_q(0))
            at(T_QB, lambda: b_q(1))
            at(T_QB, lambda: b_early(l, 2))
            at(T_B, lambda j: stage_b(l, j), NE)
            at(T_SC, lambda: row_scale(l))
            at(T_QC, lambda: c_q(l))
            at(T_EF, lambda j: e_far(l, j), NF)
            at(T_D, lambda j: stage_d(l, j))
            pl.when((t == T_ON) & (l == 0))(lambda: o_near(l))
            pl.when((t == T_OE) & (l > 0))(lambda: o_out(l))
            at(T_OE, lambda: stage_d(l, NCH - 2))
            pl.when((t == T_LN) & (l > 0))(lambda: last_near(l))
            at(T_EA, lambda j: e_all(l, j))
            at(T_OS, o_send)
            at(T_C1, lambda j: stage_c(l, j), C1)
            at(T_C2, lambda j: stage_c(l, j), C2)
            at(T_C3, lambda j: stage_c(l, j), C3)
            at(T_EN, lambda j: e_near(l, j), NF)
            at(T_OF, o_fwd)
            pl.when((t == T_LN0) & (l == 0))(lambda: last_near(l))
            pl.when((t == T_OE) & (l == 0))(lambda: o_far(l))
            at(T_ATT, lambda: attend(l))
            return carry2

        lax.fori_loop(0, STEPS, step, 0)
        last_far(l)
        return carry

    def yx(g, n):
        return rc(yx_s.at[g, n], yx_r.at[g, n], sp(sem_yx, g, n), dev_y)

    def last_rows(l, s, g):
        m = m_all[NCH - 1, g].reshape(rows // 2, CH)
        for n in (1 - y, y):
            cols = pl.ds(pl.multiple_of(n * half, half), half)
            v = acc[g, :, cols] + jnp.dot(m, wd_b[s, :, cols], preferred_element_type=F32)
            yx_s[g, n] = v.astype(BF)
            if n is y:
                pl.when(l + 1 < L)(lambda: yx(g, y).start())
            else:
                yx(g, n).start()

    @jax.named_scope("last_near")
    def last_near(l):
        j = NCH - 1
        near_in(l, j)
        last_rows(l, lax.rem(l * NCH + j, ND), own(l))

    @jax.named_scope("last_far")
    def last_far(l):
        j = NCH - 1
        i = l * NCH + j
        g = 1 - own(l)
        m_from(j, g, c, sem_mq, dev_q).wait_recv()
        m_from(j, g, 1 - c, sem_mf, dev_d).wait_recv()
        last_rows(l, lax.rem(i, ND), g)
        next_d(i)

    @jax.named_scope("swap")
    def finish():
        hr = rows // 2
        for g in range(2):
            yx(g, y).wait_recv()
            cols = pl.ds(pl.multiple_of(y * half, half), half)
            upd = yx_s[g, y].astype(F32) + yx_r[g, y].astype(F32)
            hout[g * hr:(g + 1) * hr, :] = (h_b[g, :, cols].astype(F32) + upd).astype(BF)
        last_sends(jnp.int32(L - 1))

    lax.fori_loop(0, L, layer, 0)
    finish()


def place_kernel(kn, vn, hn, kc, vc, lens, ko, vo, ho, new_b, h_b, kv_b, sem_n, sem_h, sem_in, sem_out):
    L, ns, _, hd = kc.shape
    T = 16
    pairs = [(a, l) for l in range(L) for a in range(2)]
    news = [pltpu.make_async_copy((kn, vn)[a], new_b.at[a], sem_n.at[a]) for a in range(2)]
    h_in = pltpu.make_async_copy(hn, h_b, sem_h)
    ins = [pltpu.make_async_copy((kc, vc)[a].at[l], kv_b.at[a, l], sem_in.at[a, l]) for a, l in pairs]
    outs = [pltpu.make_async_copy(kv_b.at[a, l], (ko, vo)[a].at[l], sem_out.at[a, l]) for a, l in pairs]
    for cpy in news + ins + [h_in]:
        cpy.start()
    for cpy in news:
        cpy.wait()
    row = lax.broadcasted_iota(jnp.int32, (T, hd), 0)
    for k, (a, l) in enumerate(pairs):
        ins[k].wait()
        for b in range(ns):
            base = pl.multiple_of(lens[b] // T * T, T)
            tile = kv_b[a, l, b, pl.ds(base, T), :].astype(F32)
            new = new_b[a, l, b:b + 1, :].astype(F32)
            kv_b[a, l, b, pl.ds(base, T), :] = jnp.where(row == lens[b] - base, new, tile).astype(BF)
        outs[k].start()
    h_in.wait()
    h_out = pltpu.make_async_copy(h_b, ho, sem_h)
    h_out.start()
    for cpy in outs + [h_out]:
        cpy.wait()


def solution(mesh):
    row_spec = P("dp", ("x", "yz"))
    tile_in = P(None, "x", "yz")
    tile_out = P(None, "yz", "x")
    cache_spec = P(None, ("dp", "x", "yz"))
    len_spec = P(("dp", "x", "yz"))

    def device_step(hidden, norm_gain, w_q, w_kv, w_gate, w_up, w_o, w_down, k_cache, v_cache, seq_len):
        L, k_in, q_cols = w_q.shape
        rows = hidden.shape[0]
        half = hidden.shape[1]
        kv_cols = w_kv.shape[2]
        ff = w_gate.shape[2]
        ch = CH
        nch = ff // ch
        d_out = w_o.shape[2]
        ns, cache_len, hd = k_cache.shape[1:]
        zc = q_cols + kv_cols
        dims = {"layers": L, "n_chunks": nch, "d": half * 8}
        vm = pl.BlockSpec(memory_space=pltpu.VMEM)
        anyspec = pl.BlockSpec(memory_space=pl.ANY)
        DMA = pltpu.SemaphoreType.DMA
        V = pltpu.VMEM
        h_new, k_new, v_new = pl.pallas_call(
            functools.partial(step_kernel, dims),
            out_shape=(
                jax.ShapeDtypeStruct(hidden.shape, BF),
                jax.ShapeDtypeStruct((L, ns, hd), BF),
                jax.ShapeDtypeStruct((L, ns, hd), BF),
            ),
            in_specs=[vm, vm] + [anyspec] * 8 + [pl.BlockSpec(memory_space=pltpu.SMEM)],
            out_specs=(vm, vm, vm),
            scratch_shapes=[
                V((k_in, q_cols), BF), V((k_in, kv_cols), BF),
                V((NG, k_in, ch), BF), V((NG, k_in, ch), BF),
                V((q_cols, d_out), BF), V((ND, ch, d_out), BF),
                V((ns, cache_len, hd), BF), V((ns, cache_len, hd), BF),
                V((2, 2, rows // 2, half), BF), V((2, rows // 2, d_out), BF), V((2, rows // 2, d_out), BF), V((2, rows // 2, d_out), F32),
                V((8, 128), F32), V((3, 8, 128), F32), V((8, 128), F32), V((2, 2, 16, 128), F32),
                V((nch, 2, 2, 16, 2 * ch), BF), V((nch, 2, 16, 2 * ch), BF), V((nch, 16, 2 * ch), BF),
                V((nch, 2, 2, 16, ch), BF),
                V((2, 2, 16, zc), BF), V((2, 16, zc), BF), V((16, zc), BF),
                V((2, ns, zc), BF), V((2, ns, zc), BF),
                V((2, ns, q_cols), BF), V((2, 2, 2, ns, q_cols), BF),
                V((2, 2, rows // 2, half), BF), V((2, 2, rows // 2, half), BF),
                DMA, DMA, DMA((NG,)), DMA((NG,)), DMA, DMA((ND,)), DMA, DMA,
                DMA((2, 2)), DMA((2, 3)), DMA((2, nch + 2 + NE)), DMA((2, nch + 2)),
                DMA((2, nch)), DMA((2, nch)), DMA((2, nch)),
                DMA((2,)), DMA((2,)), DMA((2,)), DMA((2,)), DMA((2,)), DMA((2, 2, 2)),
            ],
            compiler_params=pltpu.CompilerParams(
                collective_id=0, has_side_effects=True, vmem_limit_bytes=67_000_000),
            name="decode_step",
        )(hidden, norm_gain, w_q, w_kv, w_gate, w_up, w_o, w_down, k_cache, v_cache, seq_len)
        k_out, v_out, h_out = pl.pallas_call(
            place_kernel,
            out_shape=(
                jax.ShapeDtypeStruct(k_cache.shape, BF),
                jax.ShapeDtypeStruct(v_cache.shape, BF),
                jax.ShapeDtypeStruct(hidden.shape, BF),
            ),
            in_specs=[anyspec] * 5 + [pl.BlockSpec(memory_space=pltpu.SMEM)],
            out_specs=(anyspec,) * 3,
            scratch_shapes=[
                V((2, L, ns, hd), BF), V((rows, half), BF), V((2, L, ns, cache_len, hd), BF),
                DMA((2,)), DMA, DMA((2, L)), DMA((2, L)),
            ],
            compiler_params=pltpu.CompilerParams(vmem_limit_bytes=60_000_000),
            name="place_rows",
        )(k_new, v_new, h_new, k_cache, v_cache, seq_len)
        return h_out, k_out, v_out

    return jax.shard_map(
        device_step,
        mesh=mesh,
        in_specs=(row_spec, P(None, "x"), tile_in, tile_in, tile_in, tile_in, tile_out, tile_out, cache_spec, cache_spec, len_spec),
        out_specs=(row_spec, cache_spec, cache_spec),
        check_vma=False,
    )
```

```python
import functools

import jax
import jax.numpy as jnp
from jax import lax
from jax.experimental import pallas as pl
from jax.experimental.pallas import tpu as pltpu
from jax.sharding import PartitionSpec as P

NORM_EPS = 1e-6
SHRINK = 2.0 ** -64
MESH = pl.DeviceIdType.MESH
BF = jnp.bfloat16
F32 = jnp.float32

CH = 1024
NG = 7
ND = 8
NE = 3
NF = 4
T_A = (0, 1, 5, 6, 7)
T_AL = (2, 3, 4)
T_B = (1, 2, 6, 7, 8)
C1, C2, C3 = 0, 4, 5
T_C1, T_C2, T_C3 = (4, 5, 6, 7), (10,), (10, 11, 13)
T_D = (9, 10, 11, 13, 14, 15)
T_EA = (10, 11, 12, 14)
T_EN = (11, 12, 13)
T_EF = (15, 16, 17)
T_SC, T_QB, T_QC, T_ATT, T_OS, T_OF, T_OE, T_LN = 4, 0, 4, 7, 10, 14, 15, 15
T_ON, T_LN0 = 13, 14
STEPS = 18


def step_kernel(dims, hid, gain, wq, wkv, wg, wu, wo, wd, kc, vc, lens,
                hout, knew, vnew,
                wq_b, wkv_b, wg_b, wu_b, wo_b, wd_b, k_b, v_b,
                hin, h_b, u_b, acc, ss_s, ss_r, tot, sc_b,
                part, rb, ib, m_all, part_q, rb_q, ib_q, zq, yq, ob, o_all, yx_s, yx_r,
                sem_wq, sem_wkv, sem_g, sem_u, sem_wo, sem_d, sem_k, sem_v,
                sem_h, sem_ss, sem_rb, sem_ib, sem_mp, sem_mq, sem_mf,
                sem_zq, sem_oy, sem_op, sem_oq, sem_of, sem_yx):
    L, NCH, D = dims["layers"], dims["n_chunks"], dims["d"]
    HD = 256
    QC = wq_b.shape[1]
    x = lax.axis_index("x")
    y = lax.axis_index("yz")
    c = lax.rem(x, 2)
    cx = x // 2
    xp = x + 1 - 2 * c
    xq = lax.rem(x + 2, 4)
    xd = 3 - x
    dev_p, dev_q, dev_d, dev_y = {"x": xp}, {"x": xq}, {"x": xd}, {"yz": 1 - y}

    def rc(src, dst, sems, dev):
        return pltpu.make_async_remote_copy(
            src_ref=src, dst_ref=dst, send_sem=sems[0], recv_sem=sems[1],
            device_id=dev, device_id_type=MESH)

    def sp(s, *idx):
        return (s.at[(0,) + idx], s.at[(1,) + idx])

    def cp_q(l):
        return (pltpu.make_async_copy(wq.at[l], wq_b, sem_wq),
                pltpu.make_async_copy(wkv.at[l], wkv_b, sem_wkv))

    def cp_gu(i):
        l, j, s = i // NCH, lax.rem(i, NCH), lax.rem(i, NG)
        cols = pl.ds(pl.multiple_of(j * CH, CH), CH)
        return (pltpu.make_async_copy(wg.at[l, :, cols], wg_b.at[s], sem_g.at[s]),
                pltpu.make_async_copy(wu.at[l, :, cols], wu_b.at[s], sem_u.at[s]))

    def cp_d(i):
        l, j, s = i // NCH, lax.rem(i, NCH), lax.rem(i, ND)
        rows = pl.ds(pl.multiple_of(j * CH, CH), CH)
        return (pltpu.make_async_copy(wd.at[l, rows, :], wd_b.at[s], sem_d.at[s]),)

    def cp_o(l):
        return (pltpu.make_async_copy(wo.at[l], wo_b, sem_wo),)

    def cp_kv(l):
        return (pltpu.make_async_copy(kc.at[l], k_b, sem_k),
                pltpu.make_async_copy(vc.at[l], v_b, sem_v))

    def start(cs):
        for cpy in cs:
            cpy.start()

    def wait(cs):
        for cpy in cs:
            cpy.wait()

    start(cp_q(0))
    for k in range(4):
        start(cp_gu(k))

    rows = hid.shape[0]
    eye = (lax.broadcasted_iota(jnp.int32, (rows, 128), 0)
           == lax.broadcasted_iota(jnp.int32, (rows, 128), 1))

    def row_sums(h):
        ss = jnp.sum(h * h, axis=1, keepdims=True)
        row = jnp.sum(jnp.where(eye, ss, 0.0), axis=0, keepdims=True)
        return jnp.broadcast_to(row, tot.shape)

    with jax.named_scope("barrier"):
        barrier = pltpu.get_barrier_semaphore()
        for dev in (dev_p, dev_q, dev_d, dev_y):
            pl.semaphore_signal(barrier, inc=1, device_id=dev, device_id_type=MESH)
        pl.semaphore_wait(barrier, 4)

    with jax.named_scope("hx"):
        half = hid.shape[1]
        hr = rows // 2

        def h_rows(g, yy):
            return rc(hid.at[pl.ds(pl.multiple_of(g * hr, hr), hr)], hin.at[yy, g], sp(sem_h, g), dev_y)

        h_rows(1 - cx, y).start()
        h_rows(cx, y).start()
        for k in range(4, NG):
            start(cp_gu(k))
        start(cp_kv(0))
        for g in range(2):
            hin[y, g] = hid[g * hr:(g + 1) * hr]

    @jax.named_scope("first_rows")
    def first_rows(g):
        h_rows(g, 1 - y).wait_recv()
        for n in range(2):
            h_b[g, :, n * half:(n + 1) * half] = hin[n, g]

    def sums(k, dev):
        return rc(ss_s, ss_r.at[k], sp(sem_ss, k), dev)

    def send_sums():
        ss_s[...] = row_sums(h_b[...].reshape(rows, 2 * half).astype(F32))
        for k, dev in enumerate((dev_p, dev_q, dev_d)):
            sums(k, dev).start()

    def get_sums():
        for k, dev in enumerate((dev_p, dev_q, dev_d)):
            sums(k, dev).wait()
        tot[...] = (ss_s[...] + ss_r[0]) + (ss_r[1] + ss_r[2])

    def make_u(l, g):
        gall = gain[...].astype(F32)
        gl = gall[0:1]
        for k in range(1, L):
            gl = jnp.where(l == k, gall[k:k + 1], gl)
        u_b[g] = (h_b[g].astype(F32) * (gl * SHRINK)).astype(BF)

    @jax.named_scope("scale")
    def row_scale(l):
        get_sums()
        tot_col = jnp.sum(jnp.where(eye, jnp.broadcast_to(tot[0:1], eye.shape), 0.0), axis=1, keepdims=True)
        sc = jnp.broadcast_to(lax.rsqrt(tot_col / D + NORM_EPS) / SHRINK, eye.shape)
        for r in range(4):
            sc_b[r // 2, r % 2] = sc[16 * r:16 * r + 16]

    def scaled(z, g):
        sc = sc_b[g, c][:, 0:1]
        return jnp.where(sc > 0.0, z * sc, 0.0)

    def put_rows(dst, cols, val):
        v = val.astype(BF)
        for r in range(4):
            dst[r // 2, r % 2, :, cols] = v[16 * r:16 * r + 16]

    pieces = (slice(0, QC // 2), slice(QC // 2, QC + HD))

    def to_p_q(k):
        cols = pieces[k]
        return rc(part_q.at[:, 1 - c, :, cols], rb_q.at[:, :, cols], sp(sem_rb, NCH + k), dev_p)

    def to_q_q(k):
        cols = pieces[k]
        return rc(part_q.at[1 - cx, c, :, cols], ib_q.at[:, cols], sp(sem_ib, NCH + k), dev_q)

    @jax.named_scope("a_q")
    def a_q(l):
        wait(cp_q(l))
        u = u_b[...].reshape(rows, u_b.shape[2])
        for k in range(2):
            for n in range(k * QC // 2, (k + 1) * QC // 2, 512):
                put_rows(part_q, slice(n, n + 512), jnp.dot(u, wq_b[:, n:n + 512], preferred_element_type=F32))
            if k == 1:
                put_rows(part_q, slice(QC, QC + HD), jnp.dot(u, wkv_b[...], preferred_element_type=F32))
            to_p_q(k).start()

        @pl.when(l + 1 < L)
        def _():
            start(cp_q(l + 1))

    @jax.named_scope("b_q")
    def b_q(k):
        cols = pieces[k]
        to_p_q(k).wait()
        s = part_q[1 - cx, c, :, cols].astype(F32) + rb_q[1 - cx, :, cols].astype(F32)
        part_q[1 - cx, c, :, cols] = s.astype(BF)
        to_q_q(k).start()

    @jax.named_scope("c_q")
    def c_q(l):
        for k in range(2):
            to_q_q(k).wait()
        z = scaled((part_q[cx, c].astype(F32) + rb_q[cx].astype(F32)) + ib_q[...].astype(F32), cx)
        zq[0] = z[0:8].astype(BF)
        zq[1] = z[8:16].astype(BF)
        rc(zq.at[1 - y], yq.at[y], sp(sem_zq), dev_y).start()
        yq[y] = zq[y]

    @jax.named_scope("attend")
    def attend(l):
        rc(zq.at[1 - y], yq.at[1 - y], sp(sem_zq), dev_y).wait()
        q0 = yq[0].astype(F32)
        q1 = yq[1].astype(F32)
        k_new = q0[:, QC:]
        v_new = q1[:, QC:]
        knew[l] = k_new.astype(BF)
        vnew[l] = v_new.astype(BF)
        nh = QC // HD
        ns = 8
        heads = [qq[:, h * HD:(h + 1) * HD] for qq in (q0, q1) for h in range(nh)]
        qf = jnp.concatenate(heads, axis=0)
        qb = qf.astype(BF)
        nr = 2 * nh * ns
        pos = lax.broadcasted_iota(jnp.int32, (nr, HD), 1)
        seq = lax.rem(lax.broadcasted_iota(jnp.int32, (nr, HD), 0), ns)
        ln = jnp.zeros((nr, HD), jnp.int32)
        for b in range(ns):
            ln = jnp.where(seq == b, lens[b], ln)
        k_rep = jnp.concatenate([k_new] * (2 * nh), axis=0)
        v_rep = jnp.concatenate([v_new] * (2 * nh), axis=0)
        s_new = jnp.sum(qf * k_rep, axis=1, keepdims=True)
        wait(cp_kv(l))
        s = jnp.zeros((nr, HD), F32)
        for b in range(ns):
            sb = lax.dot_general(qb, k_b[b], (((1,), (1,)), ((), ())), preferred_element_type=F32)
            s = jnp.where(seq == b, sb, s)
        s = jnp.where(pos == ln, s_new, s) * HD ** -0.5
        s = jnp.where(pos <= ln, s, -1e30)
        e = jnp.exp(s - jnp.max(s, axis=1, keepdims=True))
        p = (e / jnp.sum(e, axis=1, keepdims=True)).astype(BF).astype(F32)
        p_new = jnp.sum(jnp.where(pos == ln, p, 0.0), axis=1, keepdims=True)
        p_old = jnp.where(pos == ln, 0.0, p)
        o = p_new * v_rep
        for b in range(ns):
            pb = jnp.where(seq == b, p_old, 0.0).astype(BF)
            o = o + jnp.dot(pb, v_b[b], preferred_element_type=F32)
        for hh in range(2):
            for h in range(nh):
                r0 = (hh * nh + h) * ns
                ob[hh, :, h * HD:(h + 1) * HD] = o[r0:r0 + ns].astype(BF)
        rc(ob.at[1 - y], o_all.at[cx, c, y], sp(sem_oy), dev_y).start()
        o_all[cx, c, y] = ob[y]

        @pl.when(l + 1 < L)
        def _():
            start(cp_kv(l + 1))

    @jax.named_scope("o_send")
    def o_send():
        rc(ob.at[1 - y], o_all.at[cx, c, 1 - y], sp(sem_oy), dev_y).wait()
        rc(o_all.at[cx, c], o_all.at[cx, c], sp(sem_op), dev_p).start()
        rc(o_all.at[cx, c], o_all.at[cx, c], sp(sem_oq), dev_q).start()

    @jax.named_scope("o_fwd")
    def o_fwd():
        rc(o_all.at[1 - cx, c], o_all.at[1 - cx, c], sp(sem_oq), dev_q).wait_recv()
        rc(o_all.at[1 - cx, c], o_all.at[1 - cx, c], sp(sem_of), dev_p).start()

    def o_near_in(l):
        rc(o_all.at[cx, c], o_all.at[cx, 1 - c], sp(sem_op), dev_p).wait()
        wait(cp_o(l))

    def o_far_in():
        rc(o_all.at[1 - cx, c], o_all.at[1 - cx, 1 - c], sp(sem_of), dev_p).wait()
        rc(o_all.at[cx, c], o_all.at[cx, c], sp(sem_oq), dev_q).wait_send()

    def next_o(l):
        @pl.when(l + 1 < L)
        def _():
            start(cp_o(l + 1))

    def o_rows(g):
        lhs = jnp.concatenate([o_all[g, i // 2, i % 2].astype(F32) for i in range(4)], axis=0).astype(BF)
        for n in range(0, acc.shape[2], 512):
            acc[g, :, n:n + 512] += jnp.dot(lhs, wo_b[:, n:n + 512], preferred_element_type=F32)

    @jax.named_scope("o_near")
    def o_near(l):
        o_near_in(l)
        o_rows(cx)

    @jax.named_scope("o_far")
    def o_far(l):
        o_far_in()
        o_rows(1 - cx)
        next_o(l)

    @jax.named_scope("o_all_rows")
    def o_out(l):
        o_near_in(l)
        o_far_in()
        blocks = [o_all[i // 4, (i // 2) % 2, i % 2].astype(F32) for i in range(8)]
        lhs = jnp.concatenate(blocks, axis=0).astype(BF)
        hr = rows // 2
        for n in range(0, acc.shape[2], 512):
            v = jnp.dot(lhs, wo_b[:, n:n + 512], preferred_element_type=F32)
            for g in range(2):
                acc[g, :, n:n + 512] += v[g * hr:(g + 1) * hr]
        next_o(l)

    def own(l):
        return lax.rem(cx + l, 2)

    def gu_products(l, j, u, put):
        s = lax.rem(l * NCH + j, NG)
        for n in range(0, CH, 512):
            put(slice(n, n + 512), jnp.dot(u, wg_b[s, :, n:n + 512], preferred_element_type=F32))
            put(slice(CH + n, CH + n + 512), jnp.dot(u, wu_b[s, :, n:n + 512], preferred_element_type=F32))

    def half_rows(l, j, g):
        def put(cols, val):
            v = val.astype(BF)
            for r in range(2):
                part[j, g, r, :, cols] = v[16 * r:16 * r + 16]
        gu_products(l, j, u_b[g], put)

    def next_gu(i):
        @pl.when(i + NG < L * NCH)
        def _():
            start(cp_gu(i + NG))

    def to_p(j):
        return rc(part.at[j, :, 1 - c], rb.at[j], sp(sem_rb, j), dev_p)

    def to_p_half(j, g, k):
        return rc(part.at[j, g, 1 - c], rb.at[j, g], sp(sem_rb, k), dev_p)

    def to_q(l, j):
        return rc(part.at[j, 1 - own(l), c], ib.at[j], sp(sem_ib, j), dev_q)

    @jax.named_scope("a_early")
    def a_early(l, j):
        wait(cp_gu(l * NCH + j))
        half_rows(l, j, 1 - own(l))
        to_p_half(j, 1 - own(l), j).start()

    @jax.named_scope("a_late")
    def a_late(l, j):
        half_rows(l, j, own(l))
        to_p_half(j, own(l), NCH + 2 + j).start()
        next_gu(l * NCH + j)

    @jax.named_scope("stage_a")
    def stage_a(l, j):
        i = l * NCH + j
        wait(cp_gu(i))
        dst = part.at[j]
        gu_products(l, j, u_b[...].reshape(rows, u_b.shape[2]), lambda cols, val: put_rows(dst, cols, val))
        to_p(j).start()
        next_gu(i)

    def add_to_q(l, j):
        g = 1 - own(l)
        s = part[j, g, c].astype(F32) + rb[j, g].astype(F32)
        part[j, g, c] = s.astype(BF)
        to_q(l, j).start()

    @jax.named_scope("b_early")
    def b_early(l, j):
        to_p_half(j, 1 - own(l), j).wait()
        add_to_q(l, j)

    @jax.named_scope("stage_b")
    def stage_b(l, j):
        to_p(j).wait()
        add_to_q(l, j)

    @jax.named_scope("stage_c")
    def stage_c(l, j):
        g = own(l)

        @pl.when(j < NE)
        def _():
            to_p_half(j, g, NCH + 2 + j).wait()

        to_q(l, j).wait()
        z = (part[j, g, c].astype(F32) + rb[j, g].astype(F32)) + ib[j].astype(F32)
        z = scaled(z, g).astype(BF).astype(F32)
        gate, up = z[:, :CH], z[:, CH:]
        m_all[j, g, c] = (jax.nn.silu(gate) * up).astype(BF)
        m_send(j, g, sem_mq, dev_q).start()

        @pl.when(j == NCH - 1)
        def _():
            m_send(j, g, sem_mf, dev_d).start()

        m_send(j, g, sem_mp, dev_p).start()

    def m_send(j, g, sem, dev):
        return rc(m_all.at[j, g, c], m_all.at[j, g, c], sp(sem, j), dev)

    def m_from(j, g, cc, sem, dev):
        return rc(m_all.at[j, g, cc], m_all.at[j, g, cc], sp(sem, j), dev)

    @jax.named_scope("stage_d")
    def stage_d(l, j):
        g = 1 - own(l)
        m_from(j, g, c, sem_mq, dev_q).wait_recv()
        m_send(j, g, sem_mf, dev_p).start()

    def e_rows(s, j, g):
        m = m_all[j, g].reshape(rows // 2, CH)
        for n in range(0, acc.shape[2], 512):
            acc[g, :, n:n + 512] += jnp.dot(m, wd_b[s, :, n:n + 512], preferred_element_type=F32)

    def near_in(l, j):
        m_send(j, own(l), sem_mp, dev_p).wait_send()
        m_from(j, own(l), 1 - c, sem_mp, dev_p).wait_recv()
        wait(cp_d(l * NCH + j))

    def far_in(l, j):
        g = 1 - own(l)
        m_send(j, g, sem_mf, dev_p).wait_send()
        m_from(j, g, 1 - c, sem_mf, dev_p).wait_recv()
        m_send(j, own(l), sem_mq, dev_q).wait_send()

    def next_d(i):
        @pl.when(i + ND < L * NCH)
        def _():
            start(cp_d(i + ND))

    @jax.named_scope("e_all")
    def e_all(l, j):
        i = l * NCH + j
        near_in(l, j)
        far_in(l, j)
        s = lax.rem(i, ND)
        m = m_all[j].reshape(rows, CH)
        hr = rows // 2
        for n in range(0, acc.shape[2], 512):
            v = jnp.dot(m, wd_b[s, :, n:n + 512], preferred_element_type=F32)
            for g in range(2):
                acc[g, :, n:n + 512] += v[g * hr:(g + 1) * hr]
        next_d(i)

    @jax.named_scope("e_near")
    def e_near(l, j):
        near_in(l, j)
        e_rows(lax.rem(l * NCH + j, ND), j, own(l))

    @jax.named_scope("e_far")
    def e_far(l, j):
        i = l * NCH + j
        far_in(l, j)
        e_rows(lax.rem(i, ND), j, 1 - own(l))
        next_d(i)

    @jax.named_scope("take_rows")
    def take_rows(g):
        for n in range(2):
            yx(g, n).wait_recv()
        for n in range(2):
            cols = slice(n * half, (n + 1) * half)
            upd = yx_s[g, n].astype(F32) + yx_r[g, n].astype(F32)
            h_b[g, :, cols] = (h_b[g, :, cols].astype(F32) + upd).astype(BF)

    @jax.named_scope("last_sends")
    def last_sends(l):
        j = NCH - 1
        m_send(j, own(l), sem_mq, dev_q).wait_send()
        m_send(j, own(l), sem_mf, dev_d).wait_send()
        for g in range(2):
            yx(g, 1 - y).wait_send()
            pl.when(l + 1 < L)(lambda: yx(g, y).wait_send())

    def layer(l, carry):
        early = 1 - own(l)

        pl.when(l == 0)(lambda: first_rows(early))
        pl.when(l > 0)(lambda: take_rows(early))
        make_u(l, early)
        a_early(l, 0)
        a_early(l, 1)
        b_early(l, 0)
        a_early(l, 2)
        b_early(l, 1)

        pl.when(l == 0)(lambda: first_rows(1 - early))
        pl.when(l > 0)(lambda: take_rows(1 - early))
        send_sums()
        make_u(l, 1 - early)
        a_q(l)
        acc[...] = jnp.zeros_like(acc)
        pl.when(l > 0)(lambda: last_sends(l - 1))

        @pl.when(l == 0)
        def _():
            for g in range(2):
                h_rows(g, y).wait_send()

        def step(t, carry2):
            def at(steps, fn, first=0, t=t):
                if isinstance(steps, int):
                    pl.when(t == steps)(fn)
                    return
                hit = t == steps[0]
                j = jnp.int32(first)
                for k, st in enumerate(steps[1:]):
                    hit = hit | (t == st)
                    j = jnp.where(t >= st, first + k + 1, j)
                pl.when(hit)(lambda: fn(j))

            at(T_A, lambda j: stage_a(l, j), NE)
            at(T_AL, lambda j: a_late(l, j))
            pl.when((l == 0) & (t < ND))(lambda: start(cp_d(t)))
            pl.when((l == 0) & (t == 3))(lambda: start(cp_o(0)))
            at(T_QB, lambda: b_q(0))
            at(T_QB, lambda: b_q(1))
            at(T_QB, lambda: b_early(l, 2))
            at(T_B, lambda j: stage_b(l, j), NE)
            at(T_SC, lambda: row_scale(l))
            at(T_QC, lambda: c_q(l))
            at(T_EF, lambda j: e_far(l, j), NF)
            at(T_D, lambda j: stage_d(l, j))
            pl.when((t == T_ON) & (l == 0))(lambda: o_near(l))
            pl.when((t == T_OE) & (l > 0))(lambda: o_out(l))
            at(T_OE, lambda: stage_d(l, NCH - 2))
            pl.when((t == T_LN) & (l > 0))(lambda: last_near(l))
            at(T_EA, lambda j: e_all(l, j))
            at(T_OS, o_send)
            at(T_C1, lambda j: stage_c(l, j), C1)
            at(T_C2, lambda j: stage_c(l, j), C2)
            at(T_C3, lambda j: stage_c(l, j), C3)
            at(T_EN, lambda j: e_near(l, j), NF)
            at(T_OF, o_fwd)
            pl.when((t == T_LN0) & (l == 0))(lambda: last_near(l))
            pl.when((t == T_OE) & (l == 0))(lambda: o_far(l))
            at(T_ATT, lambda: attend(l))
            return carry2

        lax.fori_loop(0, STEPS, step, 0)
        last_far(l)
        return carry

    def yx(g, n):
        return rc(yx_s.at[g, n], yx_r.at[g, n], sp(sem_yx, g, n), dev_y)

    def last_rows(l, s, g):
        m = m_all[NCH - 1, g].reshape(rows // 2, CH)
        for n in (1 - y, y):
            cols = pl.ds(pl.multiple_of(n * half, half), half)
            v = acc[g, :, cols] + jnp.dot(m, wd_b[s, :, cols], preferred_element_type=F32)
            yx_s[g, n] = v.astype(BF)
            if n is y:
                pl.when(l + 1 < L)(lambda: yx(g, y).start())
            else:
                yx(g, n).start()

    @jax.named_scope("last_near")
    def last_near(l):
        j = NCH - 1
        near_in(l, j)
        last_rows(l, lax.rem(l * NCH + j, ND), own(l))

    @jax.named_scope("last_far")
    def last_far(l):
        j = NCH - 1
        i = l * NCH + j
        g = 1 - own(l)
        m_from(j, g, c, sem_mq, dev_q).wait_recv()
        m_from(j, g, 1 - c, sem_mf, dev_d).wait_recv()
        last_rows(l, lax.rem(i, ND), g)
        next_d(i)

    @jax.named_scope("swap")
    def finish():
        hr = rows // 2
        for g in range(2):
            yx(g, y).wait_recv()
            cols = pl.ds(pl.multiple_of(y * half, half), half)
            upd = yx_s[g, y].astype(F32) + yx_r[g, y].astype(F32)
            hout[g * hr:(g + 1) * hr, :] = (h_b[g, :, cols].astype(F32) + upd).astype(BF)
        last_sends(jnp.int32(L - 1))

    lax.fori_loop(0, L, layer, 0)
    finish()


def place_kernel(kn, vn, hn, kc, vc, lens, ko, vo, ho, new_b, h_b, kv_b, sem_n, sem_h, sem_in, sem_out):
    L, ns, _, hd = kc.shape
    T = 16
    pairs = [(a, l) for l in range(L) for a in range(2)]
    news = [pltpu.make_async_copy((kn, vn)[a], new_b.at[a], sem_n.at[a]) for a in range(2)]
    h_in = pltpu.make_async_copy(hn, h_b, sem_h)
    ins = [pltpu.make_async_copy((kc, vc)[a].at[l], kv_b.at[a, l], sem_in.at[a, l]) for a, l in pairs]
    outs = [pltpu.make_async_copy(kv_b.at[a, l], (ko, vo)[a].at[l], sem_out.at[a, l]) for a, l in pairs]
    for cpy in news + ins + [h_in]:
        cpy.start()
    for cpy in news:
        cpy.wait()
    row = lax.broadcasted_iota(jnp.int32, (T, hd), 0)
    for k, (a, l) in enumerate(pairs):
        ins[k].wait()
        for b in range(ns):
            base = pl.multiple_of(lens[b] // T * T, T)
            tile = kv_b[a, l, b, pl.ds(base, T), :].astype(F32)
            new = new_b[a, l, b:b + 1, :].astype(F32)
            kv_b[a, l, b, pl.ds(base, T), :] = jnp.where(row == lens[b] - base, new, tile).astype(BF)
        outs[k].start()
    h_in.wait()
    h_out = pltpu.make_async_copy(h_b, ho, sem_h)
    h_out.start()
    for cpy in outs + [h_out]:
        cpy.wait()


def solution(mesh):
    row_spec = P("dp", ("x", "yz"))
    tile_in = P(None, "x", "yz")
    tile_out = P(None, "yz", "x")
    cache_spec = P(None, ("dp", "x", "yz"))
    len_spec = P(("dp", "x", "yz"))

    def device_step(hidden, norm_gain, w_q, w_kv, w_gate, w_up, w_o, w_down, k_cache, v_cache, seq_len):
        L, k_in, q_cols = w_q.shape
        rows = hidden.shape[0]
        half = hidden.shape[1]
        kv_cols = w_kv.shape[2]
        ff = w_gate.shape[2]
        ch = CH
        nch = ff // ch
        d_out = w_o.shape[2]
        ns, cache_len, hd = k_cache.shape[1:]
        zc = q_cols + kv_cols
        dims = {"layers": L, "n_chunks": nch, "d": half * 8}
        vm = pl.BlockSpec(memory_space=pltpu.VMEM)
        anyspec = pl.BlockSpec(memory_space=pl.ANY)
        DMA = pltpu.SemaphoreType.DMA
        V = pltpu.VMEM
        h_new, k_new, v_new = pl.pallas_call(
            functools.partial(step_kernel, dims),
            out_shape=(
                jax.ShapeDtypeStruct(hidden.shape, BF),
                jax.ShapeDtypeStruct((L, ns, hd), BF),
                jax.ShapeDtypeStruct((L, ns, hd), BF),
            ),
            in_specs=[vm, vm] + [anyspec] * 8 + [pl.BlockSpec(memory_space=pltpu.SMEM)],
            out_specs=(vm, vm, vm),
            scratch_shapes=[
                V((k_in, q_cols), BF), V((k_in, kv_cols), BF),
                V((NG, k_in, ch), BF), V((NG, k_in, ch), BF),
                V((q_cols, d_out), BF), V((ND, ch, d_out), BF),
                V((ns, cache_len, hd), BF), V((ns, cache_len, hd), BF),
                V((2, 2, rows // 2, half), BF), V((2, rows // 2, d_out), BF), V((2, rows // 2, d_out), BF), V((2, rows // 2, d_out), F32),
                V((8, 128), F32), V((3, 8, 128), F32), V((8, 128), F32), V((2, 2, 16, 128), F32),
                V((nch, 2, 2, 16, 2 * ch), BF), V((nch, 2, 16, 2 * ch), BF), V((nch, 16, 2 * ch), BF),
                V((nch, 2, 2, 16, ch), BF),
                V((2, 2, 16, zc), BF), V((2, 16, zc), BF), V((16, zc), BF),
                V((2, ns, zc), BF), V((2, ns, zc), BF),
                V((2, ns, q_cols), BF), V((2, 2, 2, ns, q_cols), BF),
                V((2, 2, rows // 2, half), BF), V((2, 2, rows // 2, half), BF),
                DMA, DMA, DMA((NG,)), DMA((NG,)), DMA, DMA((ND,)), DMA, DMA,
                DMA((2, 2)), DMA((2, 3)), DMA((2, nch + 2 + NE)), DMA((2, nch + 2)),
                DMA((2, nch)), DMA((2, nch)), DMA((2, nch)),
                DMA((2,)), DMA((2,)), DMA((2,)), DMA((2,)), DMA((2,)), DMA((2, 2, 2)),
            ],
            compiler_params=pltpu.CompilerParams(
                collective_id=0, has_side_effects=True, vmem_limit_bytes=67_000_000),
            name="decode_step",
        )(hidden, norm_gain, w_q, w_kv, w_gate, w_up, w_o, w_down, k_cache, v_cache, seq_len)
        k_out, v_out, h_out = pl.pallas_call(
            place_kernel,
            out_shape=(
                jax.ShapeDtypeStruct(k_cache.shape, BF),
                jax.ShapeDtypeStruct(v_cache.shape, BF),
                jax.ShapeDtypeStruct(hidden.shape, BF),
            ),
            in_specs=[anyspec] * 5 + [pl.BlockSpec(memory_space=pltpu.SMEM)],
            out_specs=(anyspec,) * 3,
            scratch_shapes=[
                V((2, L, ns, hd), BF), V((rows, half), BF), V((2, L, ns, cache_len, hd), BF),
                DMA((2,)), DMA, DMA((2, L)), DMA((2, L)),
            ],
            compiler_params=pltpu.CompilerParams(vmem_limit_bytes=60_000_000),
            name="place_rows",
        )(k_new, v_new, h_new, k_cache, v_cache, seq_len)
        return h_out, k_out, v_out

    return jax.shard_map(
        device_step,
        mesh=mesh,
        in_specs=(row_spec, P(None, "x"), tile_in, tile_in, tile_in, tile_in, tile_out, tile_out, cache_spec, cache_spec, len_spec),
        out_specs=(row_spec, cache_spec, cache_spec),
        check_vma=False,
    )
```
